32 devices in a mesh: dp: 4 (over y, core), seq: 2 (over x), expert: 4 (over z).
Axes of the slice: x: 2, y: 2, z: 4, core: 2. Of those that a mesh axis runs over, the one named last changes fastest.
Arguments:
- queries: bfloat16 [512, 4096], P(('dp', 'seq'), 'expert'), parts along dimension 0, may hold values from -256 to 256, as said below
- keys: bfloat16 [2048, 1024], P(('dp', 'seq'), 'expert'), parts along dimension 0, may hold values from -6 to 6
- values: bfloat16 [2048, 1024], P(('dp', 'seq'), 'expert'), parts along dimension 0, may hold values from -6 to 6
- lengths: int32 [32], P('dp'), parts along dimension 0, may hold values from 1 to 256, 512 in all
- routes: int32 [512, 2], P(('dp', 'seq', 'expert')), parts along dimension 0, may hold values from 0 to 3, all different within a row; in each aligned block of 16 rows (0 to 15, 16 to 31, ...) at most 12 rows name the same one
- gates: float32 [512, 2], P(('dp', 'seq', 'expert')), parts along dimension 0, may hold values from 0.2 to 1
- w_up: bfloat16 [4, 4096, 7168], P('expert', None, 'seq'), may hold values from -0.09375 to 0.09375
Outputs:
- expert_mix: bfloat16 [512, 7168], P(('dp', 'seq', 'expert')), parts along dimension 0
The draws below stay inside these ranges and needn't reach their ends.
There are 4 independent parts, one for each index of `dp`. The reference program is written for one: setup_inputs(seed, part) draws one part's arguments, and reference() takes and returns one part's arrays. A program takes and returns all parts, laid end to end along the dimension named above; an argument that names none is the same for every part. Nothing has to cross between parts.
Inputs may be any that keep to these rules, and one draw needn't show every extreme that they name: `queries`: A query row's values are those of a normal draw or, in some rows, a multiple of a sum of key rows. The 8 lengths sum to 512. `routes`: A row's two experts differ; among the 16 rows of one device no expert is named more than 12 times.
All inputs are finite; a program needn't handle non-finite values.
Results may differ from the reference program's by a relative error of at most 0.012.
Values may be sent and summed in bfloat16 or wider, within the bound.
A program may use at most 64 MiB of HBM per device.

```python
import math
import jax
import jax.numpy as jnp
import numpy as np
from jax import lax

D = 4096
H = 32
KVH = 8
HD = 128
EXPERTS = 4
FFW = 7168
SHARD = 256
Q_DEV = 64
NDOC = 8
LEN = 512
QTOK = 128
T_DEV = 16
CAP = 12


def base_keys(key):
    return jnp.clip(jax.random.normal(jax.random.fold_in(key, 71), (LEN, KVH * HD), jnp.float32), -6.0, 6.0)


def draw_keys(key, part):
    return base_keys(key).astype(jnp.bfloat16)


def draw_queries(key, part):
    drawn = jnp.clip(jax.random.normal(jax.random.fold_in(key, 72), (QTOK, H * HD), jnp.float32), -6.0, 6.0)
    return drawn.astype(jnp.bfloat16)


def block_levels(rng, dims, cuts, low, high):
    def one(axis_at, parts):
        heights = jax.random.uniform(jax.random.fold_in(jax.random.fold_in(rng, 6), axis_at), (parts,), jnp.float32, low / len(cuts), high / len(cuts))
        return jnp.repeat(jnp.exp(heights), dims[axis_at] // parts).reshape((-1,) + (1,) * (len(dims) - axis_at - 1))

    level = one(*cuts[0])
    for cut in cuts[1:]:
        level = level * one(*cut)
    return level


def profile(number_of, total, bound, lean):
    loads = [(1 << 20) // math.isqrt(rank ** lean) + 1 for rank in range(2, number_of + 1)]
    surplus, counts = total - bound - (number_of - 1), [1] * (number_of - 1)
    while surplus > 0:
        free = [i for i in range(number_of - 1) if counts[i] < bound]
        pool, budget = sum([loads[i] for i in free]), surplus
        for i in free:
            extra = min(bound - counts[i], max(1, budget * loads[i] // pool), surplus)
            counts[i] = counts[i] + extra
            surplus = surplus - extra
    return np.array([bound] + counts)


def ragged_sizes(own_key, number_of, total, limit, lean):
    if number_of == 2:
        one = jax.random.randint(own_key, (), max(1, total - limit), min(limit, total - 1) + 1)
        return jnp.stack([one, total - one])
    sizes = jnp.asarray(profile(number_of, total, limit, lean), jnp.int32)
    pairs = (number_of - 1) // 2
    giver, receiver = sizes[1:1 + 2 * pairs:2], sizes[2:2 + 2 * pairs:2]
    room = jnp.minimum(giver - 1, limit - receiver)
    moved = jax.random.randint(jax.random.fold_in(own_key, 1), (pairs,), 0, 1 << 20) % (room + 1)
    sizes = sizes.at[1:1 + 2 * pairs:2].set(giver - moved).at[2:2 + 2 * pairs:2].set(receiver + moved)
    return sizes[jax.random.permutation(jax.random.fold_in(own_key, 2), number_of)]


def deal_out(own_key, own, number, rows, number_of, top, bound, skew):
    sequence = jax.random.permutation(own_key, number_of)
    crowded, common = shares(number_of, rows * top, bound, skew, True), shares(number_of, rows * top, bound, skew, False)
    places = jnp.arange(number_of)

    def named(tallies, turn):
        used = int((tallies > 0).sum())
        fixed = max(1, used // 4)
        passed = fixed + (places - fixed + turn * (used - fixed)) % max(1, number_of - fixed)
        return jnp.zeros((number_of,), jnp.int32).at[sequence[jnp.where(places < fixed, places, passed)]].set(jnp.asarray(tallies, jnp.int32))

    tallies = jnp.where(number % 4 == 0, named(crowded, number // 4), named(common, number - number // 4 - 1))
    mixed = jax.random.permutation(jax.random.fold_in(own, 3), number_of)
    donor, receiver = mixed[0:number_of // 2 * 2:2], mixed[1:number_of // 2 * 2:2]
    room = jnp.minimum(tallies[donor] - 1, bound - tallies[receiver]) // 2
    room = jnp.where((donor == sequence[0]) | (receiver == sequence[0]) | (tallies[receiver] == 0), 0, jnp.maximum(room, 0))
    passed = jax.random.randint(jax.random.fold_in(own, 4), (number_of // 2,), 0, 1 << 20) % (room + 1)
    tallies = tallies.at[donor].add(-passed).at[receiver].add(passed)
    members = jnp.searchsorted(jnp.cumsum(tallies), jnp.arange(rows * top), side="right").astype(jnp.int32)
    listing = members.reshape(top, rows).T
    listing = listing[jax.random.permutation(jax.random.fold_in(own, 1), rows)]
    turn = jax.random.randint(jax.random.fold_in(own, 2), (rows, 1), 0, top)
    return jnp.take_along_axis(listing, (jnp.arange(top)[None, :] + turn) % top, axis=1)


def shares(amount, total, limit, skew, full):
    weights = [(1 << 20) // math.isqrt(standing ** skew) + 1 for standing in range(1, amount + 1)]
    largest = limit if full else min(limit, max(-(-total // amount), total * weights[0] // sum(weights)))
    least = 1 if total - largest >= amount - 1 else 0
    given, rest = [largest] + [least] * (amount - 1), total - largest - least * (amount - 1)
    while rest > 0:
        free = [i for i in range(1, amount) if given[i] < largest] or [i for i in range(1, amount) if given[i] < limit]
        whole, left = sum([weights[i] for i in free]), rest
        for i in free:
            extra = min(limit - given[i], max(1, left * weights[i] // whole), rest)
            given[i] = given[i] + extra
            rest = rest - extra
    return np.array(given)


def normal_values(key, shape, scale, bound, pieces=(), held_as=jnp.bfloat16):
    array = jax.random.normal(key, shape, jnp.float32) * scale
    if len(pieces) > 0:
        array = block_levels(key, shape, pieces, -0.22, 0.18) * array
    return jnp.clip(array, min=-bound, max=bound).astype(held_as)


def setup_inputs(seed: int = 0, part: int = 0) -> dict:
    key_of = jax.random.split(jax.random.key(seed), 8)
    part_splits = jax.random.split(jax.random.fold_in(key_of[7], part), 8)
    queries = draw_queries(jax.random.fold_in(jax.random.fold_in(key_of[7], part), 71), part)
    keys = draw_keys(jax.random.fold_in(jax.random.fold_in(key_of[7], part), 71), part)
    values = normal_values(part_splits[2], (LEN, KVH * HD), 1.0, 6.0, ((0, 2), (1, 4)))
    lengths = ragged_sizes(part_splits[3], NDOC, LEN, LEN // 2, 2).astype(jnp.int32)
    routes_keys = jax.random.split(jax.random.fold_in(part_splits[4], 1), QTOK // T_DEV)
    routes_turns = jax.random.permutation(jax.random.fold_in(part_splits[4], 3), QTOK // T_DEV)
    routes = jax.vmap(lambda own, number: deal_out(jax.random.fold_in(part_splits[4], 2), own, number, T_DEV, EXPERTS, 2, CAP, 2))(routes_keys, routes_turns).reshape((QTOK, 2))
    gates = jnp.clip(0.2 + 0.8 * jax.random.uniform(part_splits[5], (QTOK, 2), jnp.float32) ** block_levels(part_splits[5], (QTOK, 2), ((0, 8),), -0.2, 0.2), 0.2, 1.0)
    w_up = normal_values(key_of[6], (EXPERTS, D, FFW), D ** -0.5, 0.09375, ((0, 4), (2, 2)))
    return {"queries": queries, "keys": keys, "values": values, "lengths": lengths, "routes": routes, "gates": gates, "w_up": w_up}


def doc_index(positions, starts):
    return lax.optimization_barrier(jnp.sum((positions[:, None] >= starts[None, :]).astype(jnp.int32), axis=1)) - 1

def reference(queries, keys, values, lengths, routes, gates, w_up):
    qtok = queries.shape[0]
    rows = jnp.arange(qtok, dtype=jnp.int32)
    qpos = rows // Q_DEV * SHARD + SHARD - Q_DEV + rows % Q_DEV
    starts = (jnp.cumsum(lengths) - lengths).astype(jnp.int32)
    kpos = jnp.arange(LEN, dtype=jnp.int32)
    qdoc = doc_index(qpos, starts)
    kdoc = doc_index(kpos, starts)
    allowed = (kpos[None, :] <= qpos[:, None]) & (kdoc[None, :] == qdoc[:, None])
    group = H // KVH
    scale = 1.0 / HD ** 0.5
    q_heads = queries.astype(jnp.float32).reshape(qtok, KVH, group, HD).transpose(1, 2, 0, 3)
    k_heads = keys.astype(jnp.float32).reshape(LEN, KVH, HD).transpose(1, 0, 2)
    v_heads = values.astype(jnp.float32).reshape(LEN, KVH, HD).transpose(1, 0, 2)

    def one_head(operands):
        q_part, k_part, v_part = operands
        score = jnp.einsum('gqd,pd->gqp', q_part, k_part) * scale
        masked = jnp.where(allowed[None], score, jnp.float32(-1e+30))
        peak = lax.optimization_barrier(jnp.max(masked, axis=-1, keepdims=True))
        weight = jnp.where(allowed[None], jnp.exp(score - peak), jnp.float32(0.0))
        total = lax.optimization_barrier(jnp.sum(weight, axis=-1))
        weight_b = lax.optimization_barrier(weight.astype(jnp.bfloat16)).astype(jnp.float32)
        attended = jnp.einsum('gqp,pd->gqd', weight_b, v_part) / total[..., None]
        return attended.astype(jnp.bfloat16)
    heads_out = lax.map(one_head, (q_heads, k_heads, v_heads))
    attended = heads_out.transpose(2, 0, 1, 3).reshape(qtok, H * HD)
    feats = attended.astype(jnp.float32)
    normed = (feats * lax.rsqrt(lax.optimization_barrier(jnp.mean(feats * feats, axis=-1, keepdims=True)) + 1e-05)).astype(jnp.bfloat16)

    def per_expert(acc, operands):
        weight_e, which = operands
        upper = jnp.dot(normed, weight_e, preferred_element_type=jnp.float32)
        act = lax.optimization_barrier(jax.nn.silu(upper).astype(jnp.bfloat16)).astype(jnp.float32)
        share = lax.optimization_barrier(jnp.sum(jnp.where(routes == which, gates, jnp.float32(0.0)), axis=1))
        return (acc + share[:, None] * act, None)
    start_acc = jnp.zeros((qtok, FFW), jnp.float32)
    mixed, _ = lax.scan(per_expert, start_acc, (w_up, jnp.arange(EXPERTS, dtype=jnp.int32)))
    return mixed.astype(jnp.bfloat16)
```

```python
import functools

import jax
import jax.numpy as jnp
from jax import lax
from jax.experimental import pallas as pl
from jax.experimental.pallas import tpu as pltpu
from jax.sharding import PartitionSpec as P

HD = 128
MESH = pl.DeviceIdType.MESH
F32 = jnp.float32
BF16 = jnp.bfloat16
NT = (((1,), (1,)), ((), ()))


def up(n, m):
    return -(-n // m) * m


def iota(shape, dim):
    return lax.broadcasted_iota(jnp.int32, shape, dim)


def onehot(mask):
    return jnp.where(mask, F32(1.0), F32(0.0)).astype(BF16)


def dot(a, b):
    return jnp.dot(a, b, preferred_element_type=F32)


def kernel(
    cfg,
    len_hbm, q_hbm, k_hbm, v_hbm, routes_hbm, gates_hbm, w_hbm, out_ref,
    len_ref, q_ref, k_ref, v_ref, routes_ref, gates_ref,
    wbuf, kvbuf, rbuf, xbuf, acc, sendbuf, recv,
    in_sem, w_sem, kv_send, kv_recv, r_send, r_recv, z_send, z_recv, x_send, x_recv,
    b_send, b_recv,
):
    S, E, ndoc, cap, F, RP, nc, steps, pieces, tile = cfg
    s = lax.axis_index("seq")
    e = lax.axis_index("expert")
    Q, width = q_ref.shape
    shard = k_ref.shape[0]
    kvl = k_ref.shape[1] // HD
    group = width // HD // kvl
    hw = group * HD
    T = routes_ref.shape[1]
    ff = w_hbm.shape[1]
    depth = w_hbm.shape[0]
    scale = 1.0 / HD**0.5

    def at_s(d):
        return lax.rem(s + S - d, S)

    def at_e(d):
        return lax.rem(e + E - d, E)

    barrier = pltpu.get_barrier_semaphore()
    for ds in range(S):
        for de in range(E):
            if ds or de:
                pl.semaphore_signal(
                    barrier, inc=1, device_id={"seq": at_s(ds), "expert": at_e(de)},
                    device_id_type=MESH,
                )

    near = [sorted(range(E), key=lambda o, n=n: (abs(o - n), o)) for n in range(E)]
    origin = [e]
    for k in range(1, E):
        o = near[0][k]
        for n in range(1, E):
            o = jnp.where(e == n, near[n][k], o)
        origin.append(o)

    def w_copy(k):
        return pltpu.make_async_copy(
            w_hbm.at[pl.ds(pl.multiple_of(origin[k] * width, width), width)],
            wbuf.at[origin[k]], w_sem.at[k],
        )

    ins = []
    for i, (src, dst) in enumerate((
        (k_hbm, k_ref), (q_hbm, q_ref), (v_hbm, v_ref), (len_hbm, len_ref),
        (routes_hbm, routes_ref), (gates_hbm, gates_ref),
    )):
        c = pltpu.make_async_copy(src, dst, in_sem.at[i])
        c.start()
        ins.append(c)
    for c in ins[:5]:
        c.wait()

    def remote(src, dst, ssem, rsem, to_s, to_e):
        return pltpu.make_async_remote_copy(
            src_ref=src, dst_ref=dst, send_sem=ssem, recv_sem=rsem,
            device_id={"seq": to_s, "expert": to_e}, device_id_type=MESH,
        )

    def all_of(ref, sem):
        return pltpu.make_async_copy(ref, ref, sem)

    for k in range(E):
        w_copy(k).start()

    qn = group * Q
    qpos = s * shard + shard - Q + lax.rem(iota((qn, 1), 0), Q)
    docstart = jnp.zeros((qn, 1), jnp.int32)
    begin = jnp.int32(0)
    for j in range(ndoc):
        docstart = jnp.where(qpos >= begin, begin, docstart)
        begin = begin + len_ref[j]

    def masked(q, k, first):
        sc = lax.dot_general(q, k, NT, preferred_element_type=F32) * scale
        kpos = first + iota((1, k.shape[0]), 1)
        return jnp.where((kpos <= qpos) & (kpos >= docstart), sc, F32(-1e30))

    queries = []
    local = []
    for h in range(kvl):
        q = jnp.concatenate(
            [q_ref[:, (h * group + g) * HD:(h * group + g + 1) * HD] for g in range(group)], axis=0
        )
        queries.append(q)
        sc = masked(q, k_ref[:, h * HD:(h + 1) * HD], s * shard)
        peak = jnp.max(sc, axis=-1, keepdims=True)
        wt = jnp.exp(sc - peak)
        local.append((peak, jnp.sum(wt, axis=-1, keepdims=True),
                      dot(wt.astype(BF16), v_ref[:, h * HD:(h + 1) * HD])))

    pl.semaphore_wait(barrier, S * E - 1)

    spans = []
    offset = 0
    for d, first in pieces:
        spans.append((offset, shard - first))
        offset += shard - first
    for h in range(kvl):
        for i, (d, first) in enumerate(pieces):
            @pl.when(s + d < S)
            def _():
                lo, n = spans[i]
                for j, ref in enumerate((k_ref, v_ref)):
                    remote(
                        ref.at[pl.ds(first, n), pl.ds(h * HD, HD)],
                        kvbuf.at[h, j, pl.ds(lo, n)],
                        kv_send.at[i], kv_recv.at[i, h], s + d, e,
                    ).start()
    for ds in range(S):
        for de in range(E):
            if ds or de:
                remote(routes_ref, rbuf.at[ds * E + de], r_send.at[0], r_recv.at[0],
                       at_s(ds), at_e(de)).start()

    def part(h):
        return pl.ds(h * hw, hw)

    def spread(o, h, rising, falling):
        src = xbuf.at[0, o, :, part(h)]

        @pl.when(rising)
        def _():
            remote(src, src, z_send.at[0], z_recv.at[o, h], s, e + 1).start()

        @pl.when(falling)
        def _():
            remote(src, src, z_send.at[1], z_recv.at[o, h], s, e - 1).start()

        for ds in range(1, S):
            remote(src, xbuf.at[ds, o, :, part(h)], x_send.at[0], x_recv.at[ds - 1, o, h],
                   at_s(ds), e).start()

    def store_head(h, got, total):
        att = (got / total).astype(BF16)
        for g in range(group):
            cols = slice((h * group + g) * HD, (h * group + g + 1) * HD)
            xbuf[0, e, :, cols] = att[g * Q:(g + 1) * Q]

    for h in range(kvl):
        peak, total, got = local[h]

        @pl.when(s == 0)
        def _():
            store_head(h, got, total)

        @pl.when(s > 0)
        def _():
            q = queries[h]
            run_peak, run_total, run_got = peak, total, got
            for i, (d, first) in enumerate(pieces):
                lo, n = spans[i]
                if d > 1:
                    @pl.when(s < d)
                    def _():
                        kvbuf[h, :, lo:lo + n] = jnp.zeros((2, n, HD), BF16)

                @pl.when(s >= d)
                def _():
                    all_of(kvbuf.at[h, :, pl.ds(lo, n)], kv_recv.at[i, h]).wait()

                sc = masked(q, kvbuf[h, 0, lo:lo + n], (s - d) * shard + first)
                higher = jnp.maximum(run_peak, jnp.max(sc, axis=-1, keepdims=True))
                wt = jnp.exp(sc - higher)
                fade = jnp.exp(run_peak - higher)
                run_total = run_total * fade + jnp.sum(wt, axis=-1, keepdims=True)
                run_got = run_got * fade + dot(wt.astype(BF16), kvbuf[h, 1, lo:lo + n])
                run_peak = higher
            store_head(h, run_got, run_total)

        spread(e, h, e + 1 < E, e > 0)

    def squares(g, o):
        xf = xbuf[g, o].astype(F32)
        return jnp.sum(xf * xf, axis=-1, keepdims=True)

    w_copy(0).wait()
    square = squares(0, e)
    x = xbuf[0, e]
    for c0 in range(0, ff, tile):
        acc[:, c0:c0 + tile] = dot(x, wbuf[e, :, c0:c0 + tile])

    all_of(rbuf.at[pl.ds(1, S * E - 1)], r_recv.at[0]).wait()
    mine = routes_ref[...]
    names = iota((up(E, 8), 1), 0)
    upper = onehot(iota((T, T), 0) < iota((T, T), 1))

    def ranks(rt):
        mt = onehot((rt[0:1, :] == names) | (rt[1:2, :] == names))
        return mt, dot(mt, upper)

    rows_out, rows_in = E * RP, F * Q
    out_row = iota((rows_out, 1), 0)
    in_row = iota((1, rows_in), 1)
    inner = lax.rem(out_row, RP)
    to_block = lax.rem(e + E - lax.div(out_row, RP), E)
    fold = jnp.where(inner < F * cap, lax.div(inner, cap), F)
    slot = (lax.rem(inner, cap) + 1).astype(F32)
    same = (fold == lax.div(in_row, Q)) & (to_block == lax.div(lax.rem(in_row, Q), T))
    own_before = None
    perms = []
    for g in range(S):
        placed = jnp.zeros((up(E, 8), rows_in), F32)
        for de in range(E):
            mt, cnt = ranks(mine if g == 0 and de == 0 else rbuf[g * E + de])
            if own_before is None:
                own_before = cnt
            place = jnp.where(mt > 0.5, cnt + 1.0, F32(0.0)).astype(BF16)
            shift = onehot(iota((T, rows_in), 0) + lax.rem(e + de, E) * T
                           == lax.rem(iota((T, rows_in), 1), Q))
            placed = placed + dot(place, shift)
        row = jnp.sum(jnp.where(names == e, placed, F32(0.0)), axis=0, keepdims=True)
        perms.append(onehot(same & (row == slot)))

    sends = []

    def give_back(g, square, product):
        factor = lax.rsqrt(square / depth + 1e-05)
        to = at_s(S - g) if g else s
        half = (S - g) % S
        for st, (c0, n) in enumerate(steps):
            folded = []
            for f in range(F):
                part = product(slice(f * nc + c0, f * nc + c0 + n)) * factor
                folded.append((part / (1.0 + jnp.exp(-part))).astype(BF16))
            moved = dot(perms[g], jnp.concatenate(folded, axis=0)).astype(BF16)
            for de in range(E):
                block = moved[de * RP:(de + 1) * RP]
                if g or de:
                    sendbuf[g * E + de, :, c0:c0 + n] = block
                else:
                    recv[0, 0, :, c0:c0 + n] = block
            for de in reversed(range(E)):
                if g or de:
                    c = remote(sendbuf.at[g * E + de, :, pl.ds(c0, n)],
                               recv.at[half, de, :, pl.ds(c0, n)],
                               b_send.at[0], b_recv.at[half, st], to, at_e(de))
                    c.start()

    for k in range(1, E):
        o = origin[k]
        for h in range(kvl):
            all_of(xbuf.at[0, o, :, part(h)], z_recv.at[o, h]).wait()
            spread(o, h, (o < e) & (e + 1 < E), (o > e) & (e > 0))
        w_copy(k).wait()
        square = square + squares(0, o)
        x = xbuf[0, o]
        if k < E - 1:
            for c0 in range(0, ff, tile):
                acc[:, c0:c0 + tile] += dot(x, wbuf[o, :, c0:c0 + tile])
        else:
            give_back(0, square, lambda cols: acc[:, cols] + dot(x, wbuf[o, :, cols]))

    for g in range(1, S):
        square = jnp.zeros((Q, 1), F32)
        for o in range(E):
            for h in range(kvl):
                all_of(xbuf.at[g, o, :, part(h)], x_recv.at[g - 1, o, h]).wait()
            square = square + squares(g, o)

        def whole(cols, g=g):
            total = dot(xbuf[g, 0], wbuf[0, :, cols])
            for o in range(1, E):
                total = total + dot(xbuf[g, o], wbuf[o, :, cols])
            return total

        give_back(g, square, whole)

    ins[5].wait()
    diagonal = iota((T, T), 0) == iota((T, T), 1)

    def column(row):
        return jnp.sum(jnp.where(diagonal, row, jnp.zeros_like(row)), axis=1, keepdims=True)

    wide = iota((T, E * RP), 1)
    at = []
    for k in range(2):
        rk = mine[k:k + 1, :]
        rank = jnp.sum(jnp.where(rk == names, own_before, F32(0.0)), axis=0, keepdims=True)
        rel = rk - e
        rel = jnp.where(rel < 0, rel + E, rel)
        at.append(column((rel * RP).astype(F32) + rank).astype(jnp.int32))
    pick = jnp.concatenate(
        [onehot(at[k] + f * cap == wide) for f in range(F) for k in range(2)], axis=0
    )
    g0, g1 = column(gates_ref[0:1, :]), column(gates_ref[1:2, :])

    for half in range(S):
        base = lax.rem(s + half, S) * ff
        for st, (c0, n) in enumerate(steps):
            came = recv.at[half, pl.ds(0 if half else 1, E if half else E - 1), :, pl.ds(c0, n)]
            all_of(came, b_recv.at[half, st]).wait()
            got = recv[half, :, :, c0:c0 + n].reshape(E * RP, n)
            res = dot(pick, got)
            for f in range(F):
                lo = 2 * f * T
                mix = g0 * res[lo:lo + T] + g1 * res[lo + T:lo + 2 * T]
                cols = pl.ds(pl.multiple_of(base + f * nc + c0, 128), n)
                out_ref[:, cols] = mix.astype(BF16)

    for i, (d, first) in enumerate(pieces):
        @pl.when(s + d < S)
        def _():
            lo, n = spans[i]
            all_of(kvbuf.at[:, :, pl.ds(lo, n)], kv_send.at[i]).wait()
    all_of(rbuf.at[pl.ds(1, S * E - 1)], r_send.at[0]).wait()
    for n in range(E):
        @pl.when(e == n)
        def _():
            if n + 1 < E:
                all_of(xbuf.at[0, pl.ds(0, n + 1)], z_send.at[0]).wait()
            if n > 0:
                all_of(xbuf.at[0, pl.ds(0, E - n)], z_send.at[1]).wait()
    all_of(xbuf.at[pl.ds(0, S - 1)], x_send.at[0]).wait()
    all_of(sendbuf.at[pl.ds(0, S * E - 1)], b_send.at[0]).wait()


def shards(queries, keys, values, lengths, routes, gates, w_up):
    S, E = lax.axis_size("seq"), lax.axis_size("expert")
    q_rows, width = queries.shape
    shard = keys.shape[0]
    w = w_up.reshape(w_up.shape[1], w_up.shape[2])
    depth, ff = w.shape
    T = routes.shape[0]
    cap = max(2, 3 * q_rows // (E * E))
    choices = [f for f in range(1, ff // 128 + 1) if ff % (f * 128) == 0]
    F = min(choices, key=lambda f: up(f * cap, 16) * (ff // f))
    RP = up(F * cap, 16)
    nc = ff // F
    cuts = list(range(0, max(nc - 255, 1), 256))
    steps = [(c, (cuts + [nc])[i + 1] - c) for i, c in enumerate(cuts)]
    tile = 512 if ff % 512 == 0 else 128
    window = shard * S // 2
    pieces = []
    for d in range(1, S):
        first = max(0, (d + 1) * shard - q_rows - window + 1) // 16 * 16
        if first < shard:
            pieces.append((d, first))
    kv_rows = sum(shard - first for _, first in pieces)
    cfg = (S, E, lengths.shape[0], cap, F, RP, nc, steps, pieces, tile)
    kvl = keys.shape[1] // HD
    dma = pltpu.SemaphoreType.DMA
    args = [
        pltpu.with_memory_space_constraint(a, pltpu.HBM)
        for a in (lengths, queries, keys, values, routes.T, gates.T, w)
    ]
    return pl.pallas_call(
        functools.partial(kernel, cfg),
        out_shape=pltpu.VMEM((T, S * ff), BF16),
        in_specs=[pl.BlockSpec(memory_space=pltpu.HBM)] * 7,
        out_specs=pl.BlockSpec(memory_space=pltpu.VMEM),
        scratch_shapes=[
            pltpu.SMEM(lengths.shape, jnp.int32),
            pltpu.VMEM(queries.shape, BF16),
            pltpu.VMEM(keys.shape, BF16),
            pltpu.VMEM(values.shape, BF16),
            pltpu.VMEM((2, T), jnp.int32),
            pltpu.VMEM((2, T), F32),
            pltpu.VMEM((E, width, ff), BF16),
            pltpu.VMEM((kvl, 2, kv_rows, HD), BF16),
            pltpu.VMEM((S * E, 2, T), jnp.int32),
            pltpu.VMEM((S, E, q_rows, width), BF16),
            pltpu.VMEM((q_rows, ff), F32),
            pltpu.VMEM((S * E, RP, nc), BF16),
            pltpu.VMEM((S, E, RP, nc), BF16),
            dma((6,)),
            dma((E,)),
            dma((len(pieces),)),
            dma((len(pieces), kvl)),
            dma((1,)), dma((1,)),
            dma((2,)), dma((E, kvl)),
            dma((1,)), dma((S - 1, E, kvl)),
            dma((1,)), dma((S, len(steps))),
        ],
        compiler_params=pltpu.CompilerParams(
            collective_id=0, has_side_effects=True, vmem_limit_bytes=60 * 1024 * 1024
        ),
    )(*args)


def solution(mesh):
    placed = (
        P(("dp", "seq"), "expert"),
        P(("dp", "seq"), "expert"),
        P(("dp", "seq"), "expert"),
        P("dp"),
        P(("dp", "seq", "expert"), None),
        P(("dp", "seq", "expert"), None),
        P("expert", None, "seq"),
    )
    return jax.shard_map(
        shards,
        mesh=mesh,
        in_specs=placed,
        out_specs=P(("dp", "seq", "expert"), None),
        check_vma=False,
    )
```

```python
import functools

import jax
import jax.numpy as jnp
from jax import lax
from jax.experimental import pallas as pl
from jax.experimental.pallas import tpu as pltpu
from jax.sharding import PartitionSpec as P

HD = 128
MESH = pl.DeviceIdType.MESH
F32 = jnp.float32
BF16 = jnp.bfloat16
NT = (((1,), (1,)), ((), ()))


def up(n, m):
    return -(-n // m) * m


def iota(shape, dim):
    return lax.broadcasted_iota(jnp.int32, shape, dim)


def onehot(mask):
    return jnp.where(mask, F32(1.0), F32(0.0)).astype(BF16)


def dot(a, b):
    return jnp.dot(a, b, preferred_element_type=F32)


def kernel(
    cfg,
    len_hbm, q_hbm, k_hbm, v_hbm, routes_hbm, gates_hbm, w_hbm, out_ref,
    len_ref, q_ref, k_ref, v_ref, routes_ref, gates_ref,
    wbuf, kvbuf, rbuf, pack, xbuf, acc, sendbuf, recv,
    in_sem, w_sem, kv_send, kv_recv, r_send, r_recv, z_send, z_recv, x_send, x_recv,
    b_send, b_recv,
):
    S, E, ndoc, cap, RB, F, RP, nc, steps, pieces, tile = cfg
    s = lax.axis_index("seq")
    e = lax.axis_index("expert")
    Q, width = q_ref.shape
    shard = k_ref.shape[0]
    kvl = k_ref.shape[1] // HD
    group = width // HD // kvl
    hw = group * HD
    T = routes_ref.shape[1]
    ff = w_hbm.shape[1]
    depth = w_hbm.shape[0]
    scale = 1.0 / HD**0.5

    def at_s(d):
        return lax.rem(s + S - d, S)

    def at_e(d):
        return lax.rem(e + E - d, E)

    barrier = pltpu.get_barrier_semaphore()
    for ds in range(S):
        for de in range(E):
            if ds or de:
                pl.semaphore_signal(
                    barrier, inc=1, device_id={"seq": at_s(ds), "expert": at_e(de)},
                    device_id_type=MESH,
                )

    near = [sorted(range(E), key=lambda o, n=n: (abs(o - n), o)) for n in range(E)]
    origin = [e]
    for k in range(1, E):
        o = near[0][k]
        for n in range(1, E):
            o = jnp.where(e == n, near[n][k], o)
        origin.append(o)

    def w_copy(k):
        return pltpu.make_async_copy(
            w_hbm.at[pl.ds(pl.multiple_of(origin[k] * width, width), width)],
            wbuf.at[origin[k]], w_sem.at[k],
        )

    ins = []
    for i, (src, dst) in enumerate((
        (k_hbm, k_ref), (q_hbm, q_ref), (v_hbm, v_ref), (len_hbm, len_ref),
        (routes_hbm, routes_ref), (gates_hbm, gates_ref),
    )):
        c = pltpu.make_async_copy(src, dst, in_sem.at[i])
        c.start()
        ins.append(c)
    for c in ins[:5]:
        c.wait()

    def remote(src, dst, ssem, rsem, to_s, to_e):
        return pltpu.make_async_remote_copy(
            src_ref=src, dst_ref=dst, send_sem=ssem, recv_sem=rsem,
            device_id={"seq": to_s, "expert": to_e}, device_id_type=MESH,
        )

    def all_of(ref, sem):
        return pltpu.make_async_copy(ref, ref, sem)

    for k in range(E):
        w_copy(k).start()

    qn = group * Q
    qpos = s * shard + shard - Q + lax.rem(iota((qn, 1), 0), Q)
    docstart = jnp.zeros((qn, 1), jnp.int32)
    begin = jnp.int32(0)
    for j in range(ndoc):
        docstart = jnp.where(qpos >= begin, begin, docstart)
        begin = begin + len_ref[j]

    def masked(q, k, first):
        sc = lax.dot_general(q, k, NT, preferred_element_type=F32) * scale
        kpos = first + iota((1, k.shape[0]), 1)
        return jnp.where((kpos <= qpos) & (kpos >= docstart), sc, F32(-1e30))

    queries = []
    local = []
    for h in range(kvl):
        q = jnp.concatenate(
            [q_ref[:, (h * group + g) * HD:(h * group + g + 1) * HD] for g in range(group)], axis=0
        )
        queries.append(q)
        sc = masked(q, k_ref[:, h * HD:(h + 1) * HD], s * shard)
        peak = jnp.max(sc, axis=-1, keepdims=True)
        wt = jnp.exp(sc - peak)
        local.append((peak, jnp.sum(wt, axis=-1, keepdims=True),
                      dot(wt.astype(BF16), v_ref[:, h * HD:(h + 1) * HD])))

    pl.semaphore_wait(barrier, S * E - 1)

    spans = []
    offset = 0
    for d, first in pieces:
        spans.append((offset, shard - first))
        offset += shard - first
    for h in range(kvl):
        for i, (d, first) in enumerate(pieces):
            @pl.when(s + d < S)
            def _():
                lo, n = spans[i]
                for j, ref in enumerate((k_ref, v_ref)):
                    remote(
                        ref.at[pl.ds(first, n), pl.ds(h * HD, HD)],
                        kvbuf.at[h, j, pl.ds(lo, n)],
                        kv_send.at[i], kv_recv.at[i, h], s + d, e,
                    ).start()
    for de in range(1, E):
        remote(routes_ref, rbuf.at[de], r_send.at[0], r_recv.at[0], s, at_e(de)).start()

    def part(h):
        return pl.ds(h * hw, hw)

    def relay(src, o, h):
        for ds in range(1, S):
            remote(src, xbuf.at[ds, o, :, part(h)], x_send.at[0], x_recv.at[ds - 1, o, h],
                   at_s(ds), e).start()

    all_of(rbuf.at[pl.ds(1, E - 1)], r_recv.at[0]).wait()
    mine = routes_ref[...]
    names = iota((up(E, 8), 1), 0)
    upper = onehot(iota((T, T), 0) < iota((T, T), 1))
    total_place = jnp.zeros((up(E, 8), Q), F32)
    for de in range(E):
        rt = mine if de == 0 else rbuf[de]
        mt = onehot((rt[0:1, :] == names) | (rt[1:2, :] == names))
        cnt = dot(mt, upper)
        blk = lax.rem(e + de, E)
        place = jnp.where(mt > 0.5, cnt + (blk * cap).astype(F32) + 1.0, F32(0.0))
        if de == 0:
            before = cnt
        shift = onehot(iota((T, Q), 0) + blk * T == iota((T, Q), 1))
        total_place = total_place + dot(place.astype(BF16), shift)
    row_of = iota((RB, Q), 0).astype(F32) + 1.0
    selector = jnp.concatenate(
        [onehot(total_place[x:x + 1, :] == row_of) for x in range(E)], axis=0
    )

    def store_head(h, got, total):
        att = (got / total).astype(BF16)
        for g in range(group):
            cols = slice((h * group + g) * HD, (h * group + g + 1) * HD)
            packed = dot(selector, att[g * Q:(g + 1) * Q]).astype(BF16)
            for x in range(E):
                pack[x, :, cols] = packed[x * RB:(x + 1) * RB]

    for h in range(kvl):
        peak, total, got = local[h]

        @pl.when(s == 0)
        def _():
            store_head(h, got, total)

        @pl.when(s > 0)
        def _():
            q = queries[h]
            run_peak, run_total, run_got = peak, total, got
            for i, (d, first) in enumerate(pieces):
                lo, n = spans[i]
                if d > 1:
                    @pl.when(s < d)
                    def _():
                        kvbuf[h, :, lo:lo + n] = jnp.zeros((2, n, HD), BF16)

                @pl.when(s >= d)
                def _():
                    all_of(kvbuf.at[h, :, pl.ds(lo, n)], kv_recv.at[i, h]).wait()

                sc = masked(q, kvbuf[h, 0, lo:lo + n], (s - d) * shard + first)
                higher = jnp.maximum(run_peak, jnp.max(sc, axis=-1, keepdims=True))
                wt = jnp.exp(sc - higher)
                fade = jnp.exp(run_peak - higher)
                run_total = run_total * fade + jnp.sum(wt, axis=-1, keepdims=True)
                run_got = run_got * fade + dot(wt.astype(BF16), kvbuf[h, 1, lo:lo + n])
                run_peak = higher
            store_head(h, run_got, run_total)

        for k in range(1, E):
            to = origin[k]
            remote(pack.at[to, :, part(h)], xbuf.at[0, e, :, part(h)],
                   z_send.at[0], z_recv.at[e, h], s, to).start()
        relay(pack.at[e, :, part(h)], e, h)


    def squares(g, o):
        xf = xbuf[g, o].astype(F32)
        return jnp.sum(xf * xf, axis=-1, keepdims=True)

    w_copy(0).wait()
    xbuf[0, e] = pack[e]
    square = squares(0, e)
    x = xbuf[0, e]
    for c0 in range(0, ff, tile):
        acc[:, c0:c0 + tile] = dot(x, wbuf[e, :, c0:c0 + tile])

    rows_out, rows_in = E * RP, F * RB
    out_row = iota((rows_out, 1), 0)
    inner = lax.rem(out_row, RP)
    e_of = lax.rem(e + E - lax.div(out_row, RP), E)
    from_row = lax.div(inner, cap) * RB + e_of * cap + lax.rem(inner, cap)
    from_row = jnp.where(inner < F * cap, from_row, -1)
    perm = onehot(from_row == iota((rows_out, rows_in), 1))

    def give_back(g, square, product):
        factor = lax.rsqrt(square / depth + 1e-05)
        to = at_s(S - g) if g else s
        half = (S - g) % S
        for st, (c0, n) in enumerate(steps):
            folded = []
            for f in range(F):
                part = product(slice(f * nc + c0, f * nc + c0 + n)) * factor
                folded.append((part / (1.0 + jnp.exp(-part))).astype(BF16))
            moved = dot(perm, jnp.concatenate(folded, axis=0)).astype(BF16)
            for de in range(E):
                block = moved[de * RP:(de + 1) * RP]
                if g or de:
                    sendbuf[g * E + de, :, c0:c0 + n] = block
                else:
                    recv[0, 0, :, c0:c0 + n] = block
            for de in reversed(range(E)):
                if g or de:
                    c = remote(sendbuf.at[g * E + de, :, pl.ds(c0, n)],
                               recv.at[half, de, :, pl.ds(c0, n)],
                               b_send.at[0], b_recv.at[half, st], to, at_e(de))
                    c.start()

    for k in range(1, E):
        o = origin[k]
        for h in range(kvl):
            all_of(xbuf.at[0, o, :, part(h)], z_recv.at[o, h]).wait()
            relay(xbuf.at[0, o, :, part(h)], o, h)
        w_copy(k).wait()
        square = square + squares(0, o)
        x = xbuf[0, o]
        if k < E - 1:
            for c0 in range(0, ff, tile):
                acc[:, c0:c0 + tile] += dot(x, wbuf[o, :, c0:c0 + tile])
        else:
            give_back(0, square, lambda cols: acc[:, cols] + dot(x, wbuf[o, :, cols]))

    for g in range(1, S):
        square = jnp.zeros((RB, 1), F32)
        for o in range(E):
            for h in range(kvl):
                all_of(xbuf.at[g, o, :, part(h)], x_recv.at[g - 1, o, h]).wait()
            square = square + squares(g, o)

        def whole(cols, g=g):
            total = dot(xbuf[g, 0], wbuf[0, :, cols])
            for o in range(1, E):
                total = total + dot(xbuf[g, o], wbuf[o, :, cols])
            return total

        give_back(g, square, whole)

    ins[5].wait()
    diagonal = iota((T, T), 0) == iota((T, T), 1)

    def column(row):
        return jnp.sum(jnp.where(diagonal, row, jnp.zeros_like(row)), axis=1, keepdims=True)

    wide = iota((T, E * RP), 1)
    at = []
    for k in range(2):
        rk = mine[k:k + 1, :]
        rank = jnp.sum(jnp.where(rk == names, before, F32(0.0)), axis=0, keepdims=True)
        rel = rk - e
        rel = jnp.where(rel < 0, rel + E, rel)
        at.append(column((rel * RP).astype(F32) + rank).astype(jnp.int32))
    pick = jnp.concatenate(
        [onehot(at[k] + f * cap == wide) for f in range(F) for k in range(2)], axis=0
    )
    g0, g1 = column(gates_ref[0:1, :]), column(gates_ref[1:2, :])

    for half in range(S):
        base = lax.rem(s + half, S) * ff
        for st, (c0, n) in enumerate(steps):
            came = recv.at[half, pl.ds(0 if half else 1, E if half else E - 1), :, pl.ds(c0, n)]
            all_of(came, b_recv.at[half, st]).wait()
            got = recv[half, :, :, c0:c0 + n].reshape(E * RP, n)
            res = dot(pick, got)
            for f in range(F):
                lo = 2 * f * T
                mix = g0 * res[lo:lo + T] + g1 * res[lo + T:lo + 2 * T]
                cols = pl.ds(pl.multiple_of(base + f * nc + c0, 128), n)
                out_ref[:, cols] = mix.astype(BF16)

    for i, (d, first) in enumerate(pieces):
        @pl.when(s + d < S)
        def _():
            lo, n = spans[i]
            all_of(kvbuf.at[:, :, pl.ds(lo, n)], kv_send.at[i]).wait()
    all_of(rbuf.at[pl.ds(1, E - 1)], r_send.at[0]).wait()
    all_of(pack.at[pl.ds(0, E - 1)], z_send.at[0]).wait()
    all_of(xbuf.at[pl.ds(0, S - 1)], x_send.at[0]).wait()
    all_of(sendbuf.at[pl.ds(0, S * E - 1)], b_send.at[0]).wait()


def shards(queries, keys, values, lengths, routes, gates, w_up):
    S, E = lax.axis_size("seq"), lax.axis_size("expert")
    q_rows, width = queries.shape
    shard = keys.shape[0]
    w = w_up.reshape(w_up.shape[1], w_up.shape[2])
    depth, ff = w.shape
    T = routes.shape[0]
    cap = max(2, 3 * q_rows // (E * E))
    choices = [f for f in range(1, ff // 128 + 1) if ff % (f * 128) == 0]
    RB = up(E * cap, 16)
    F = min(choices, key=lambda f: up(f * cap, 16) * (ff // f))
    RP = up(F * cap, 16)
    nc = ff // F
    cuts = list(range(0, max(nc - 255, 1), 256))
    steps = [(c, (cuts + [nc])[i + 1] - c) for i, c in enumerate(cuts)]
    tile = 512 if ff % 512 == 0 else 128
    window = shard * S // 2
    pieces = []
    for d in range(1, S):
        first = max(0, (d + 1) * shard - q_rows - window + 1) // 16 * 16
        if first < shard:
            pieces.append((d, first))
    kv_rows = sum(shard - first for _, first in pieces)
    cfg = (S, E, lengths.shape[0], cap, RB, F, RP, nc, steps, pieces, tile)
    kvl = keys.shape[1] // HD
    dma = pltpu.SemaphoreType.DMA
    args = [
        pltpu.with_memory_space_constraint(a, pltpu.HBM)
        for a in (lengths, queries, keys, values, routes.T, gates.T, w)
    ]
    return pl.pallas_call(
        functools.partial(kernel, cfg),
        out_shape=pltpu.VMEM((T, S * ff), BF16),
        in_specs=[pl.BlockSpec(memory_space=pltpu.HBM)] * 7,
        out_specs=pl.BlockSpec(memory_space=pltpu.VMEM),
        scratch_shapes=[
            pltpu.SMEM(lengths.shape, jnp.int32),
            pltpu.VMEM(queries.shape, BF16),
            pltpu.VMEM(keys.shape, BF16),
            pltpu.VMEM(values.shape, BF16),
            pltpu.VMEM((2, T), jnp.int32),
            pltpu.VMEM((2, T), F32),
            pltpu.VMEM((E, width, ff), BF16),
            pltpu.VMEM((kvl, 2, kv_rows, HD), BF16),
            pltpu.VMEM((E, 2, T), jnp.int32),
            pltpu.VMEM((E, RB, width), BF16),
            pltpu.VMEM((S, E, RB, width), BF16),
            pltpu.VMEM((RB, ff), F32),
            pltpu.VMEM((S * E, RP, nc), BF16),
            pltpu.VMEM((S, E, RP, nc), BF16),
            dma((6,)),
            dma((E,)),
            dma((len(pieces),)),
            dma((len(pieces), kvl)),
            dma((1,)), dma((1,)),
            dma((1,)), dma((E, kvl)),
            dma((1,)), dma((S - 1, E, kvl)),
            dma((1,)), dma((S, len(steps))),
        ],
        compiler_params=pltpu.CompilerParams(
            collective_id=0, has_side_effects=True, vmem_limit_bytes=60 * 1024 * 1024
        ),
    )(*args)


def solution(mesh):
    placed = (
        P(("dp", "seq"), "expert"),
        P(("dp", "seq"), "expert"),
        P(("dp", "seq"), "expert"),
        P("dp"),
        P(("dp", "seq", "expert"), None),
        P(("dp", "seq", "expert"), None),
        P("expert", None, "seq"),
    )
    return jax.shard_map(
        shards,
        mesh=mesh,
        in_specs=placed,
        out_specs=P(("dp", "seq", "expert"), None),
        check_vma=False,
    )
```

```python
import functools

import jax
import jax.numpy as jnp
from jax import lax
from jax.experimental import pallas as pl
from jax.experimental.pallas import tpu as pltpu
from jax.sharding import PartitionSpec as P

HD = 128
MESH = pl.DeviceIdType.MESH
F32 = jnp.float32
BF16 = jnp.bfloat16
NT = (((1,), (1,)), ((), ()))


def up(n, m):
    return -(-n // m) * m


def iota(shape, dim):
    return lax.broadcasted_iota(jnp.int32, shape, dim)


def onehot(mask):
    return jnp.where(mask, F32(1.0), F32(0.0)).astype(BF16)


def dot(a, b):
    return jnp.dot(a, b, preferred_element_type=F32)


def kernel(
    cfg,
    len_hbm, q_hbm, k_hbm, v_hbm, routes_hbm, gates_hbm, w_hbm, out_ref,
    len_ref, q_ref, k_ref, v_ref, routes_ref, gates_ref,
    wbuf, kvbuf, rbuf, raw, nbuf, fwd, sel_ref, pack, xbuf, acc, square_ref, sendbuf, recv,
    in_sem, w_sem, kv_send, kv_recv, r_send, r_recv, z_send, z_recv, x_send, x_recv,
    b_send, b_recv, n_recv,
):
    S, E, ndoc, cap, RB, F, RP, nc, steps, pieces, tile = cfg
    s = lax.axis_index("seq")
    e = lax.axis_index("expert")
    Q, width = q_ref.shape
    shard = k_ref.shape[0]
    kvl = k_ref.shape[1] // HD
    group = width // HD // kvl
    hw = group * HD
    T = routes_ref.shape[1]
    ff = w_hbm.shape[1]
    depth = w_hbm.shape[0]
    scale = 1.0 / HD**0.5

    def at_s(d):
        return lax.rem(s + S - d, S)

    def at_e(d):
        return lax.rem(e + E - d, E)

    barrier = pltpu.get_barrier_semaphore()
    for ds in range(S):
        for de in range(E):
            if (ds == 0) != (de == 0):
                pl.semaphore_signal(
                    barrier, inc=1, device_id={"seq": at_s(ds), "expert": at_e(de)},
                    device_id_type=MESH,
                )

    mid = (E // 2 - 1, E // 2)

    def key(n, o):
        return (o != n, not (n in mid and o in mid), abs(o - n), o)

    near = [sorted(range(E), key=functools.partial(key, n)) for n in range(E)]
    origin = [e]
    for k in range(1, E):
        o = near[0][k]
        for n in range(1, E):
            o = jnp.where(e == n, near[n][k], o)
        origin.append(o)

    inner_dev = (e == mid[0]) | (e == mid[1])
    side = lax.div(e, E // 2)
    across = E - 1 - e

    def w_copy(k):
        return pltpu.make_async_copy(
            w_hbm.at[pl.ds(pl.multiple_of(origin[k] * width, width), width)],
            wbuf.at[origin[k]], w_sem.at[k],
        )

    ins = []
    for i, (src, dst) in enumerate((
        (k_hbm, k_ref), (q_hbm, q_ref), (v_hbm, v_ref), (len_hbm, len_ref),
        (routes_hbm, routes_ref), (gates_hbm, gates_ref),
    )):
        c = pltpu.make_async_copy(src, dst, in_sem.at[i])
        c.start()
        ins.append(c)
    for c in ins[:5]:
        c.wait()

    def remote(src, dst, ssem, rsem, to_s, to_e):
        return pltpu.make_async_remote_copy(
            src_ref=src, dst_ref=dst, send_sem=ssem, recv_sem=rsem,
            device_id={"seq": to_s, "expert": to_e}, device_id_type=MESH,
        )

    def all_of(ref, sem):
        return pltpu.make_async_copy(ref, ref, sem)

    for k in range(E):
        w_copy(k).start()

    qn = group * Q
    qpos = s * shard + shard - Q + lax.rem(iota((qn, 1), 0), Q)
    docstart = jnp.zeros((qn, 1), jnp.int32)
    begin = jnp.int32(0)
    for j in range(ndoc):
        docstart = jnp.where(qpos >= begin, begin, docstart)
        begin = begin + len_ref[j]

    def masked(q, k, first):
        sc = lax.dot_general(q, k, NT, preferred_element_type=F32) * scale
        kpos = first + iota((1, k.shape[0]), 1)
        return jnp.where((kpos <= qpos) & (kpos >= docstart), sc, F32(-1e30))

    queries = []
    local = []
    for h in range(kvl):
        q = jnp.concatenate(
            [q_ref[:, (h * group + g) * HD:(h * group + g + 1) * HD] for g in range(group)], axis=0
        )
        queries.append(q)
        sc = masked(q, k_ref[:, h * HD:(h + 1) * HD], s * shard)
        peak = jnp.max(sc, axis=-1, keepdims=True)
        wt = jnp.exp(sc - peak)
        local.append((peak, jnp.sum(wt, axis=-1, keepdims=True),
                      dot(wt.astype(BF16), v_ref[:, h * HD:(h + 1) * HD])))

    pl.semaphore_wait(barrier, S + E - 2)

    spans = []
    offset = 0
    for d, first in pieces:
        spans.append((offset, shard - first))
        offset += shard - first
    for h in range(kvl):
        for i, (d, first) in enumerate(pieces):
            @pl.when(s + d < S)
            def _():
                lo, n = spans[i]
                for j, ref in enumerate((k_ref, v_ref)):
                    remote(
                        ref.at[pl.ds(first, n), pl.ds(h * HD, HD)],
                        kvbuf.at[h, j, pl.ds(lo, n)],
                        kv_send.at[i], kv_recv.at[i, h], s + d, e,
                    ).start()
    for de in range(1, E):
        remote(routes_ref, rbuf.at[de], r_send.at[0], r_recv.at[0], s, at_e(de)).start()

    def part(h):
        return pl.ds(h * hw, hw)

    def relay(src, o, h):
        for ds in range(1, S):
            remote(src, xbuf.at[ds, o, :, part(h)], x_send.at[0], x_recv.at[ds - 1, o, h],
                   at_s(ds), e).start()

    def store_head(h, got, total):
        att = (got / total).astype(BF16)
        for g in range(group):
            cols = slice((h * group + g) * HD, (h * group + g + 1) * HD)
            raw[:, cols] = att[g * Q:(g + 1) * Q]

        @pl.when(inner_dev)
        def _():
            remote(raw.at[:, part(h)], nbuf.at[:, part(h)], z_send.at[1], n_recv.at[h],
                   s, across).start()

    @pl.when(s == 0)
    def _():
        for h in range(kvl):
            store_head(h, local[h][2], local[h][1])

    all_of(rbuf.at[pl.ds(1, E - 1)], r_recv.at[0]).wait()
    mine = routes_ref[...]
    names = iota((up(E, 8), 1), 0)
    upper = onehot(iota((T, T), 0) < iota((T, T), 1))
    total_place = jnp.zeros((up(E, 8), Q), F32)
    for de in range(E):
        rt = mine if de == 0 else rbuf[de]
        mt = onehot((rt[0:1, :] == names) | (rt[1:2, :] == names))
        cnt = dot(mt, upper)
        blk = lax.rem(e + de, E)
        place = jnp.where(mt > 0.5, cnt + (blk * cap).astype(F32) + 1.0, F32(0.0))
        if de == 0:
            before = cnt
        shift = onehot(iota((T, Q), 0) + blk * T == iota((T, Q), 1))
        total_place = total_place + dot(place.astype(BF16), shift)
    row_of = iota((RB, Q), 0).astype(F32) + 1.0
    chosen = [onehot(total_place[x:x + 1, :] == row_of) for x in range(E)]
    selector = jnp.concatenate(chosen, axis=0)
    for x in range(E):
        sel_ref[x] = chosen[x]

    def send(k, h):
        to = origin[k]

        @pl.when(jnp.logical_not(inner_dev) | (lax.div(to, E // 2) == side))
        def _():
            remote(pack.at[to, :, part(h)], xbuf.at[0, e, :, part(h)],
                   z_send.at[0], z_recv.at[e, h], s, to).start()

    for h in range(kvl):
        peak, total, got = local[h]

        @pl.when(s > 0)
        def _():
            q = queries[h]
            run_peak, run_total, run_got = peak, total, got
            for i, (d, first) in enumerate(pieces):
                lo, n = spans[i]
                if d > 1:
                    @pl.when(s < d)
                    def _():
                        kvbuf[h, :, lo:lo + n] = jnp.zeros((2, n, HD), BF16)

                @pl.when(s >= d)
                def _():
                    all_of(kvbuf.at[h, :, pl.ds(lo, n)], kv_recv.at[i, h]).wait()

                sc = masked(q, kvbuf[h, 0, lo:lo + n], (s - d) * shard + first)
                higher = jnp.maximum(run_peak, jnp.max(sc, axis=-1, keepdims=True))
                wt = jnp.exp(sc - higher)
                fade = jnp.exp(run_peak - higher)
                run_total = run_total * fade + jnp.sum(wt, axis=-1, keepdims=True)
                run_got = run_got * fade + dot(wt.astype(BF16), kvbuf[h, 1, lo:lo + n])
                run_peak = higher
            store_head(h, run_got, run_total)

        packed = dot(selector, raw[:, h * hw:(h + 1) * hw]).astype(BF16)
        for x in range(E):
            pack[x, :, h * hw:(h + 1) * hw] = packed[x * RB:(x + 1) * RB]
        if h == 0:
            for k in range(1, E - 1):
                send(k, h)
        relay(pack.at[e, :, part(h)], e, h)
    for k in range(1, E):
        for h in range(kvl):
            if h or k == E - 1:
                send(k, h)

    def take_across(o, h):
        all_of(nbuf.at[:, part(h)], n_recv.at[h]).wait()
        rows = nbuf[:, h * hw:(h + 1) * hw]
        for j in range(1, E // 2):
            to = side * (E // 2) + lax.rem(e + j, E // 2)
            fwd[j - 1, :, h * hw:(h + 1) * hw] = dot(sel_ref[to], rows).astype(BF16)
            remote(fwd.at[j - 1, :, part(h)], xbuf.at[0, o, :, part(h)],
                   z_send.at[2], z_recv.at[o, h], s, to).start()
        xbuf[0, o, :, h * hw:(h + 1) * hw] = dot(sel_ref[e], rows).astype(BF16)

    def squares(g, o):
        xf = xbuf[g, o].astype(F32)
        return jnp.sum(xf * xf, axis=-1, keepdims=True)

    square_ref[...] = jnp.zeros_like(square_ref)

    def gather(g, k):
        o = origin[k]
        for h in range(kvl):
            if g:
                all_of(xbuf.at[g, o, :, part(h)], x_recv.at[g - 1, o, h]).wait()
            elif k:
                def direct(o=o, h=h):
                    all_of(xbuf.at[0, o, :, part(h)], z_recv.at[o, h]).wait()

                if k == 1:
                    pl.when(inner_dev)(functools.partial(take_across, o, h))
                    pl.when(jnp.logical_not(inner_dev))(direct)
                else:
                    direct()
                relay(xbuf.at[0, o, :, part(h)], o, h)
        square_ref[g] += squares(g, o)

    def slice_of(g, k):
        if g == 0:
            w_copy(k).wait()
        o = origin[k]
        x = xbuf[g, o]
        for c0 in range(0, ff, tile):
            got = dot(x, wbuf[o, :, c0:c0 + tile])
            acc[g, :, c0:c0 + tile] = got if k == 0 else acc[g, :, c0:c0 + tile] + got

    xbuf[0, e] = pack[e]
    gather(0, 0)
    slice_of(0, 0)

    rows_out, rows_in = E * RP, F * RB
    out_row = iota((rows_out, 1), 0)
    inner = lax.rem(out_row, RP)
    e_of = lax.rem(e + E - lax.div(out_row, RP), E)
    from_row = lax.div(inner, cap) * RB + e_of * cap + lax.rem(inner, cap)
    from_row = jnp.where(inner < F * cap, from_row, -1)
    perm = onehot(from_row == iota((rows_out, rows_in), 1))

    last = list(range(max(1, E - 2), E))

    def give_back(g):
        factor = lax.rsqrt(square_ref[g] / depth + 1e-05)
        xs = [xbuf[g, origin[k]] for k in last]

        def product(cols):
            total = dot(xs[0], wbuf[origin[last[0]], :, cols])
            for x, k in zip(xs[1:], last[1:]):
                total = total + dot(x, wbuf[origin[k], :, cols])
            return total + acc[g, :, cols]

        to = at_s(S - g) if g else s
        half = (S - g) % S
        for st, (c0, n) in enumerate(steps):
            folded = []
            for f in range(F):
                part = product(slice(f * nc + c0, f * nc + c0 + n)) * factor
                folded.append((part / (1.0 + jnp.exp(-part))).astype(BF16))
            moved = dot(perm, jnp.concatenate(folded, axis=0)).astype(BF16)
            for de in range(E):
                block = moved[de * RP:(de + 1) * RP]
                if g or de:
                    sendbuf[g * E + de, :, c0:c0 + n] = block
                else:
                    recv[0, 0, :, c0:c0 + n] = block
            for de in reversed(range(E)):
                if g or de:
                    c = remote(sendbuf.at[g * E + de, :, pl.ds(c0, n)],
                               recv.at[half, de, :, pl.ds(c0, n)],
                               b_send.at[0], b_recv.at[half, st], to, at_e(de))
                    c.start()

    def others(k):
        for g in range(1, S):
            gather(g, k)
            slice_of(g, k)

    def middle():
        for k in range(1, last[0]):
            others(k)

    for k in range(1, last[0]):
        gather(0, k)
        slice_of(0, k)
        if k == 1:
            others(0)
    if last[0] == 1:
        others(0)
    pl.when(jnp.logical_not(inner_dev))(middle)
    for k in last[:-1]:
        gather(0, k)
    gather(0, last[-1])
    for k in last:
        w_copy(k).wait()
    pl.when((s == 0) | jnp.logical_not(inner_dev))(functools.partial(give_back, 0))
    pl.when(inner_dev)(middle)
    for g in range(1, S):
        for k in last:
            gather(g, k)
        give_back(g)
    pl.when((s > 0) & inner_dev)(functools.partial(give_back, 0))

    ins[5].wait()
    diagonal = iota((T, T), 0) == iota((T, T), 1)

    def column(row):
        return jnp.sum(jnp.where(diagonal, row, jnp.zeros_like(row)), axis=1, keepdims=True)

    wide = iota((T, E * RP), 1)
    at = []
    for k in range(2):
        rk = mine[k:k + 1, :]
        rank = jnp.sum(jnp.where(rk == names, before, F32(0.0)), axis=0, keepdims=True)
        rel = rk - e
        rel = jnp.where(rel < 0, rel + E, rel)
        at.append(column((rel * RP).astype(F32) + rank).astype(jnp.int32))
    pick = jnp.concatenate(
        [onehot(at[k] + f * cap == wide) for f in range(F) for k in range(2)], axis=0
    )
    g0, g1 = column(gates_ref[0:1, :]), column(gates_ref[1:2, :])

    for half in range(S):
        base = lax.rem(s + half, S) * ff
        for st, (c0, n) in enumerate(steps):
            came = recv.at[half, pl.ds(0 if half else 1, E if half else E - 1), :, pl.ds(c0, n)]
            all_of(came, b_recv.at[half, st]).wait()
            got = recv[half, :, :, c0:c0 + n].reshape(E * RP, n)
            res = dot(pick, got)
            for f in range(F):
                lo = 2 * f * T
                mix = g0 * res[lo:lo + T] + g1 * res[lo + T:lo + 2 * T]
                cols = pl.ds(pl.multiple_of(base + f * nc + c0, 128), n)
                out_ref[:, cols] = mix.astype(BF16)

    for i, (d, first) in enumerate(pieces):
        @pl.when(s + d < S)
        def _():
            lo, n = spans[i]
            all_of(kvbuf.at[:, :, pl.ds(lo, n)], kv_send.at[i]).wait()
    all_of(rbuf.at[pl.ds(1, E - 1)], r_send.at[0]).wait()

    @pl.when(jnp.logical_not(inner_dev))
    def _():
        all_of(pack.at[pl.ds(0, E - 1)], z_send.at[0]).wait()

    @pl.when(inner_dev)
    def _():
        all_of(raw, z_send.at[1]).wait()
        if E > 2:
            all_of(pack.at[pl.ds(0, E // 2 - 1)], z_send.at[0]).wait()
            all_of(fwd, z_send.at[2]).wait()

    all_of(xbuf.at[pl.ds(0, S - 1)], x_send.at[0]).wait()
    all_of(sendbuf.at[pl.ds(0, S * E - 1)], b_send.at[0]).wait()


def shards(queries, keys, values, lengths, routes, gates, w_up):
    S, E = lax.axis_size("seq"), lax.axis_size("expert")
    q_rows, width = queries.shape
    shard = keys.shape[0]
    w = w_up.reshape(w_up.shape[1], w_up.shape[2])
    depth, ff = w.shape
    T = routes.shape[0]
    cap = max(2, 3 * q_rows // (E * E))
    choices = [f for f in range(1, ff // 128 + 1) if ff % (f * 128) == 0]
    RB = up(E * cap, 16)
    F = min(choices, key=lambda f: up(f * cap, 16) * (ff // f))
    RP = up(F * cap, 16)
    nc = ff // F
    cuts = list(range(0, max(nc - 255, 1), 256))
    steps = [(c, (cuts + [nc])[i + 1] - c) for i, c in enumerate(cuts)]
    tile = 512 if ff % 512 == 0 else 128
    window = shard * S // 2
    pieces = []
    for d in range(1, S):
        first = max(0, (d + 1) * shard - q_rows - window + 1) // 16 * 16
        if first < shard:
            pieces.append((d, first))
    kv_rows = sum(shard - first for _, first in pieces)
    cfg = (S, E, lengths.shape[0], cap, RB, F, RP, nc, steps, pieces, tile)
    kvl = keys.shape[1] // HD
    dma = pltpu.SemaphoreType.DMA
    args = [
        pltpu.with_memory_space_constraint(a, pltpu.HBM)
        for a in (lengths, queries, keys, values, routes.T, gates.T, w)
    ]
    return pl.pallas_call(
        functools.partial(kernel, cfg),
        out_shape=pltpu.VMEM((T, S * ff), BF16),
        in_specs=[pl.BlockSpec(memory_space=pltpu.HBM)] * 7,
        out_specs=pl.BlockSpec(memory_space=pltpu.VMEM),
        scratch_shapes=[
            pltpu.SMEM(lengths.shape, jnp.int32),
            pltpu.VMEM(queries.shape, BF16),
            pltpu.VMEM(keys.shape, BF16),
            pltpu.VMEM(values.shape, BF16),
            pltpu.VMEM((2, T), jnp.int32),
            pltpu.VMEM((2, T), F32),
            pltpu.VMEM((E, width, ff), BF16),
            pltpu.VMEM((kvl, 2, kv_rows, HD), BF16),
            pltpu.VMEM((E, 2, T), jnp.int32),
            pltpu.VMEM(queries.shape, BF16),
            pltpu.VMEM(queries.shape, BF16),
            pltpu.VMEM((max(1, E // 2 - 1), RB, width), BF16),
            pltpu.VMEM((E, RB, q_rows), BF16),
            pltpu.VMEM((E, RB, width), BF16),
            pltpu.VMEM((S, E, RB, width), BF16),
            pltpu.VMEM((S, RB, ff), F32),
            pltpu.VMEM((S, RB, 1), F32),
            pltpu.VMEM((S * E, RP, nc), BF16),
            pltpu.VMEM((S, E, RP, nc), BF16),
            dma((6,)),
            dma((E,)),
            dma((len(pieces),)),
            dma((len(pieces), kvl)),
            dma((1,)), dma((1,)),
            dma((3,)), dma((E, kvl)),
            dma((1,)), dma((S - 1, E, kvl)),
            dma((1,)), dma((S, len(steps))), dma((kvl,)),
        ],
        compiler_params=pltpu.CompilerParams(
            collective_id=0, has_side_effects=True, vmem_limit_bytes=60 * 1024 * 1024
        ),
    )(*args)


def solution(mesh):
    placed = (
        P(("dp", "seq"), "expert"),
        P(("dp", "seq"), "expert"),
        P(("dp", "seq"), "expert"),
        P("dp"),
        P(("dp", "seq", "expert"), None),
        P(("dp", "seq", "expert"), None),
        P("expert", None, "seq"),
    )
    return jax.shard_map(
        shards,
        mesh=mesh,
        in_specs=placed,
        out_specs=P(("dp", "seq", "expert"), None),
        check_vma=False,
    )
```

```python
import functools

import jax
import jax.numpy as jnp
from jax import lax
from jax.experimental import pallas as pl
from jax.experimental.pallas import tpu as pltpu
from jax.sharding import PartitionSpec as P

HD = 128
MESH = pl.DeviceIdType.MESH
F32 = jnp.float32
BF16 = jnp.bfloat16
NT = (((1,), (1,)), ((), ()))


def up(n, m):
    return -(-n // m) * m


def iota(shape, dim):
    return lax.broadcasted_iota(jnp.int32, shape, dim)


def onehot(mask):
    return jnp.where(mask, F32(1.0), F32(0.0)).astype(BF16)


def dot(a, b):
    return jnp.dot(a, b, preferred_element_type=F32)


def kernel(
    cfg,
    len_hbm, q_hbm, k_hbm, v_hbm, routes_hbm, gates_hbm, w_hbm, out_ref,
    len_ref, q_ref, k_ref, v_ref, routes_ref, gates_ref,
    wbuf, kvbuf, rbuf, raw, nbuf, fwd, sel_ref, pack, xbuf, acc, square_ref, sendbuf, recv,
    in_sem, w_sem, kv_send, kv_recv, r_send, r_recv, z_send, z_recv, x_send, x_recv,
    b_send, b_recv, n_recv,
):
    S, E, ndoc, cap, RB, F, RP, nc, steps, pieces, tile = cfg
    s = lax.axis_index("seq")
    e = lax.axis_index("expert")
    Q, width = q_ref.shape
    shard = k_ref.shape[0]
    kvl = k_ref.shape[1] // HD
    group = width // HD // kvl
    hw = group * HD
    T = routes_ref.shape[1]
    ff = w_hbm.shape[1]
    depth = w_hbm.shape[0]
    scale = 1.0 / HD**0.5

    def at_s(d):
        return lax.rem(s + S - d, S)

    def at_e(d):
        return lax.rem(e + E - d, E)

    barrier = pltpu.get_barrier_semaphore()
    for ds in range(S):
        for de in range(E):
            if (ds == 0) != (de == 0):
                pl.semaphore_signal(
                    barrier, inc=1, device_id={"seq": at_s(ds), "expert": at_e(de)},
                    device_id_type=MESH,
                )

    mid = (E // 2 - 1, E // 2)

    def key(n, o):
        return (o != n, not (n in mid and o in mid), abs(o - n), o)

    near = [sorted(range(E), key=functools.partial(key, n)) for n in range(E)]
    origin = [e]
    for k in range(1, E):
        o = near[0][k]
        for n in range(1, E):
            o = jnp.where(e == n, near[n][k], o)
        origin.append(o)

    inner_dev = (e == mid[0]) | (e == mid[1])
    side = lax.div(e, E // 2)
    across = E - 1 - e

    def w_copy(k):
        return pltpu.make_async_copy(
            w_hbm.at[pl.ds(pl.multiple_of(origin[k] * width, width), width)],
            wbuf.at[origin[k]], w_sem.at[k],
        )

    ins = []
    for i, (src, dst) in enumerate((
        (k_hbm, k_ref), (q_hbm, q_ref), (v_hbm, v_ref), (len_hbm, len_ref),
        (routes_hbm, routes_ref), (gates_hbm, gates_ref),
    )):
        c = pltpu.make_async_copy(src, dst, in_sem.at[i])
        c.start()
        ins.append(c)
    for c in ins[:5]:
        c.wait()

    def remote(src, dst, ssem, rsem, to_s, to_e):
        return pltpu.make_async_remote_copy(
            src_ref=src, dst_ref=dst, send_sem=ssem, recv_sem=rsem,
            device_id={"seq": to_s, "expert": to_e}, device_id_type=MESH,
        )

    def all_of(ref, sem):
        return pltpu.make_async_copy(ref, ref, sem)

    for k in range(E):
        w_copy(k).start()

    qn = group * Q
    qpos = s * shard + shard - Q + lax.rem(iota((qn, 1), 0), Q)
    docstart = jnp.zeros((qn, 1), jnp.int32)
    begin = jnp.int32(0)
    for j in range(ndoc):
        docstart = jnp.where(qpos >= begin, begin, docstart)
        begin = begin + len_ref[j]

    def masked(q, k, first):
        sc = lax.dot_general(q, k, NT, preferred_element_type=F32) * scale
        kpos = first + iota((1, k.shape[0]), 1)
        return jnp.where((kpos <= qpos) & (kpos >= docstart), sc, F32(-1e30))

    queries = []
    local = []
    for h in range(kvl):
        q = jnp.concatenate(
            [q_ref[:, (h * group + g) * HD:(h * group + g + 1) * HD] for g in range(group)], axis=0
        )
        queries.append(q)
        sc = masked(q, k_ref[:, h * HD:(h + 1) * HD], s * shard)
        peak = jnp.max(sc, axis=-1, keepdims=True)
        wt = jnp.exp(sc - peak)
        local.append((peak, jnp.sum(wt, axis=-1, keepdims=True),
                      dot(wt.astype(BF16), v_ref[:, h * HD:(h + 1) * HD])))

    pl.semaphore_wait(barrier, S + E - 2)

    spans = []
    offset = 0
    for d, first in pieces:
        spans.append((offset, shard - first))
        offset += shard - first
    for h in range(kvl):
        for i, (d, first) in enumerate(pieces):
            @pl.when(s + d < S)
            def _():
                lo, n = spans[i]
                for j, ref in enumerate((k_ref, v_ref)):
                    remote(
                        ref.at[pl.ds(first, n), pl.ds(h * HD, HD)],
                        kvbuf.at[h, j, pl.ds(lo, n)],
                        kv_send.at[i], kv_recv.at[i, h], s + d, e,
                    ).start()
    for de in range(1, E):
        remote(routes_ref, rbuf.at[de], r_send.at[0], r_recv.at[0], s, at_e(de)).start()

    def part(h):
        return pl.ds(h * hw, hw)

    def relay(src, o, h):
        for ds in range(1, S):
            remote(src, xbuf.at[ds, o, :, part(h)], x_send.at[0], x_recv.at[ds - 1, o, h],
                   at_s(ds), e).start()

    def store_head(h, got, total):
        att = (got / total).astype(BF16)
        for g in range(group):
            cols = slice((h * group + g) * HD, (h * group + g + 1) * HD)
            raw[:, cols] = att[g * Q:(g + 1) * Q]

        @pl.when(inner_dev)
        def _():
            remote(raw.at[:, part(h)], nbuf.at[:, part(h)], z_send.at[1], n_recv.at[h],
                   s, across).start()

    @pl.when(s == 0)
    def _():
        for h in range(kvl):
            store_head(h, local[h][2], local[h][1])

    all_of(rbuf.at[pl.ds(1, E - 1)], r_recv.at[0]).wait()
    mine = routes_ref[...]
    names = iota((up(E, 8), 1), 0)
    upper = onehot(iota((T, T), 0) < iota((T, T), 1))
    total_place = jnp.zeros((up(E, 8), Q), F32)
    for de in range(E):
        rt = mine if de == 0 else rbuf[de]
        mt = onehot((rt[0:1, :] == names) | (rt[1:2, :] == names))
        cnt = dot(mt, upper)
        blk = lax.rem(e + de, E)
        place = jnp.where(mt > 0.5, cnt + (blk * cap).astype(F32) + 1.0, F32(0.0))
        if de == 0:
            before = cnt
        shift = onehot(iota((T, Q), 0) + blk * T == iota((T, Q), 1))
        total_place = total_place + dot(place.astype(BF16), shift)
    row_of = iota((RB, Q), 0).astype(F32) + 1.0
    chosen = [onehot(total_place[x:x + 1, :] == row_of) for x in range(E)]
    selector = jnp.concatenate(chosen, axis=0)
    for x in range(E):
        sel_ref[x] = chosen[x]

    def send(k, h):
        to = origin[k]

        @pl.when(jnp.logical_not(inner_dev) | (lax.div(to, E // 2) == side))
        def _():
            remote(pack.at[to, :, part(h)], xbuf.at[0, e, :, part(h)],
                   z_send.at[0], z_recv.at[e, h], s, to).start()

    for h in range(kvl):
        peak, total, got = local[h]

        @pl.when(s > 0)
        def _():
            q = queries[h]
            run_peak, run_total, run_got = peak, total, got
            for i, (d, first) in enumerate(pieces):
                lo, n = spans[i]
                if d > 1:
                    @pl.when(s < d)
                    def _():
                        kvbuf[h, :, lo:lo + n] = jnp.zeros((2, n, HD), BF16)

                @pl.when(s >= d)
                def _():
                    all_of(kvbuf.at[h, :, pl.ds(lo, n)], kv_recv.at[i, h]).wait()

                sc = masked(q, kvbuf[h, 0, lo:lo + n], (s - d) * shard + first)
                higher = jnp.maximum(run_peak, jnp.max(sc, axis=-1, keepdims=True))
                wt = jnp.exp(sc - higher)
                fade = jnp.exp(run_peak - higher)
                run_total = run_total * fade + jnp.sum(wt, axis=-1, keepdims=True)
                run_got = run_got * fade + dot(wt.astype(BF16), kvbuf[h, 1, lo:lo + n])
                run_peak = higher
            store_head(h, run_got, run_total)

        packed = dot(selector, raw[:, h * hw:(h + 1) * hw]).astype(BF16)
        for x in range(E):
            pack[x, :, h * hw:(h + 1) * hw] = packed[x * RB:(x + 1) * RB]
        if h == 0:
            for k in range(1, E - 1):
                send(k, h)
        relay(pack.at[e, :, part(h)], e, h)
    for k in range(1, E):
        for h in range(kvl):
            if h or k == E - 1:
                send(k, h)

    def take_across(o, h):
        all_of(nbuf.at[:, part(h)], n_recv.at[h]).wait()
        rows = nbuf[:, h * hw:(h + 1) * hw]
        for j in range(1, E // 2):
            to = side * (E // 2) + lax.rem(e + j, E // 2)
            fwd[j - 1, :, h * hw:(h + 1) * hw] = dot(sel_ref[to], rows).astype(BF16)
            remote(fwd.at[j - 1, :, part(h)], xbuf.at[0, o, :, part(h)],
                   z_send.at[2], z_recv.at[o, h], s, to).start()
        xbuf[0, o, :, h * hw:(h + 1) * hw] = dot(sel_ref[e], rows).astype(BF16)

    def squares(g, o):
        xf = xbuf[g, o].astype(F32)
        return jnp.sum(xf * xf, axis=-1, keepdims=True)

    square_ref[...] = jnp.zeros_like(square_ref)

    def gather(g, k):
        o = origin[k]
        for h in range(kvl):
            if g:
                all_of(xbuf.at[g, o, :, part(h)], x_recv.at[g - 1, o, h]).wait()
            elif k:
                def direct(o=o, h=h):
                    all_of(xbuf.at[0, o, :, part(h)], z_recv.at[o, h]).wait()

                if k == 1:
                    pl.when(inner_dev)(functools.partial(take_across, o, h))
                    pl.when(jnp.logical_not(inner_dev))(direct)
                else:
                    direct()
                relay(xbuf.at[0, o, :, part(h)], o, h)
        square_ref[g] += squares(g, o)

    def slice_of(g, k):
        if g == 0:
            w_copy(k).wait()
        o = origin[k]
        x = xbuf[g, o]
        for c0 in range(0, ff, tile):
            got = dot(x, wbuf[o, :, c0:c0 + tile])
            acc[g, :, c0:c0 + tile] += got

    xbuf[0, e] = pack[e]
    gather(0, 0)

    rows_out, rows_in = E * RP, F * RB
    out_row = iota((rows_out, 1), 0)
    inner = lax.rem(out_row, RP)
    e_of = lax.rem(e + E - lax.div(out_row, RP), E)
    from_row = lax.div(inner, cap) * RB + e_of * cap + lax.rem(inner, cap)
    from_row = jnp.where(inner < F * cap, from_row, -1)
    perm = onehot(from_row == iota((rows_out, rows_in), 1))

    last = list(range(max(1, E - 2), E))

    def give_back(g):
        factor = lax.rsqrt(square_ref[g] / depth + 1e-05)
        xs = [xbuf[g, origin[k]] for k in last]

        def product(cols):
            total = dot(xs[0], wbuf[origin[last[0]], :, cols])
            for x, k in zip(xs[1:], last[1:]):
                total = total + dot(x, wbuf[origin[k], :, cols])
            return total + acc[g, :, cols]

        to = at_s(S - g) if g else s
        half = (S - g) % S
        for st, (c0, n) in enumerate(steps):
            folded = []
            for f in range(F):
                part = product(slice(f * nc + c0, f * nc + c0 + n)) * factor
                folded.append((part / (1.0 + jnp.exp(-part))).astype(BF16))
            moved = dot(perm, jnp.concatenate(folded, axis=0)).astype(BF16)
            for de in range(E):
                block = moved[de * RP:(de + 1) * RP]
                if g or de:
                    sendbuf[g * E + de, :, c0:c0 + n] = block
                else:
                    recv[0, 0, :, c0:c0 + n] = block
            for de in reversed(range(E)):
                if g or de:
                    c = remote(sendbuf.at[g * E + de, :, pl.ds(c0, n)],
                               recv.at[half, de, :, pl.ds(c0, n)],
                               b_send.at[0], b_recv.at[half, st], to, at_e(de))
                    c.start()

    def others(k):
        for g in range(1, S):
            gather(g, k)
            slice_of(g, k)

    def own_slices(first):
        for g in range(1, S):
            gather(g, 0)
        w_copy(0).wait()
        x = jnp.concatenate([xbuf[g, e] for g in range(S)], axis=0)
        for c0 in range(0, ff, tile):
            got = dot(x, wbuf[e, :, c0:c0 + tile])
            for g in range(S):
                block = got[g * RB:(g + 1) * RB]
                if first or g:
                    acc[g, :, c0:c0 + tile] = block
                else:
                    acc[g, :, c0:c0 + tile] += block

    def middle():
        for k in range(1, last[0]):
            others(k)

    for k in range(1, last[0]):
        gather(0, k)
        if k == 1:
            w_copy(k).wait()
            o = origin[k]
            for c0 in range(0, ff, tile):
                acc[0, :, c0:c0 + tile] = dot(xbuf[0, o], wbuf[o, :, c0:c0 + tile])
            own_slices(False)
        else:
            slice_of(0, k)
    if last[0] == 1:
        own_slices(True)
    pl.when(jnp.logical_not(inner_dev))(middle)
    for k in last[:-1]:
        gather(0, k)
    gather(0, last[-1])
    for k in last:
        w_copy(k).wait()
    pl.when((s == 0) | jnp.logical_not(inner_dev))(functools.partial(give_back, 0))
    pl.when(inner_dev)(middle)
    for g in range(1, S):
        for k in last:
            gather(g, k)
        give_back(g)
    pl.when((s > 0) & inner_dev)(functools.partial(give_back, 0))

    ins[5].wait()
    diagonal = iota((T, T), 0) == iota((T, T), 1)

    def column(row):
        return jnp.sum(jnp.where(diagonal, row, jnp.zeros_like(row)), axis=1, keepdims=True)

    wide = iota((T, E * RP), 1)
    at = []
    for k in range(2):
        rk = mine[k:k + 1, :]
        rank = jnp.sum(jnp.where(rk == names, before, F32(0.0)), axis=0, keepdims=True)
        rel = rk - e
        rel = jnp.where(rel < 0, rel + E, rel)
        at.append(column((rel * RP).astype(F32) + rank).astype(jnp.int32))
    pick = jnp.concatenate(
        [onehot(at[k] + f * cap == wide) for f in range(F) for k in range(2)], axis=0
    )
    g0, g1 = column(gates_ref[0:1, :]), column(gates_ref[1:2, :])

    for owner in range(S):
        half = lax.rem(owner + S - s, S)
        for st, (c0, n) in enumerate(steps):
            @pl.when(s == owner)
            def _():
                all_of(recv.at[0, pl.ds(1, E - 1), :, pl.ds(c0, n)], b_recv.at[0, st]).wait()

            @pl.when(s != owner)
            def _():
                all_of(recv.at[half, :, :, pl.ds(c0, n)], b_recv.at[half, st]).wait()

            got = recv[half, :, :, c0:c0 + n].reshape(E * RP, n)
            res = dot(pick, got)
            for f in range(F):
                lo = 2 * f * T
                mix = g0 * res[lo:lo + T] + g1 * res[lo + T:lo + 2 * T]
                cols = slice(owner * ff + f * nc + c0, owner * ff + f * nc + c0 + n)
                out_ref[:, cols] = mix.astype(BF16)

    for i, (d, first) in enumerate(pieces):
        @pl.when(s + d < S)
        def _():
            lo, n = spans[i]
            all_of(kvbuf.at[:, :, pl.ds(lo, n)], kv_send.at[i]).wait()
    all_of(rbuf.at[pl.ds(1, E - 1)], r_send.at[0]).wait()

    @pl.when(jnp.logical_not(inner_dev))
    def _():
        all_of(pack.at[pl.ds(0, E - 1)], z_send.at[0]).wait()

    @pl.when(inner_dev)
    def _():
        all_of(raw, z_send.at[1]).wait()
        if E > 2:
            all_of(pack.at[pl.ds(0, E // 2 - 1)], z_send.at[0]).wait()
            all_of(fwd, z_send.at[2]).wait()

    all_of(xbuf.at[pl.ds(0, S - 1)], x_send.at[0]).wait()
    all_of(sendbuf.at[pl.ds(0, S * E - 1)], b_send.at[0]).wait()


def shards(queries, keys, values, lengths, routes, gates, w_up):
    S, E = lax.axis_size("seq"), lax.axis_size("expert")
    q_rows, width = queries.shape
    shard = keys.shape[0]
    w = w_up.reshape(w_up.shape[1], w_up.shape[2])
    depth, ff = w.shape
    T = routes.shape[0]
    cap = max(2, 3 * q_rows // (E * E))
    choices = [f for f in range(1, ff // 128 + 1) if ff % (f * 128) == 0]
    RB = up(E * cap, 16)
    F = min(choices, key=lambda f: up(f * cap, 16) * (ff // f))
    RP = up(F * cap, 16)
    nc = ff // F
    cuts = list(range(0, max(nc - 255, 1), 256))
    steps = [(c, (cuts + [nc])[i + 1] - c) for i, c in enumerate(cuts)]
    tile = 512 if ff % 512 == 0 else 128
    window = shard * S // 2
    pieces = []
    for d in range(1, S):
        first = max(0, (d + 1) * shard - q_rows - window + 1) // 16 * 16
        if first < shard:
            pieces.append((d, first))
    kv_rows = sum(shard - first for _, first in pieces)
    cfg = (S, E, lengths.shape[0], cap, RB, F, RP, nc, steps, pieces, tile)
    kvl = keys.shape[1] // HD
    dma = pltpu.SemaphoreType.DMA
    args = [
        pltpu.with_memory_space_constraint(a, pltpu.HBM)
        for a in (lengths, queries, keys, values, routes.T, gates.T, w)
    ]
    return pl.pallas_call(
        functools.partial(kernel, cfg),
        out_shape=pltpu.VMEM((T, S * ff), BF16),
        in_specs=[pl.BlockSpec(memory_space=pltpu.HBM)] * 7,
        out_specs=pl.BlockSpec(memory_space=pltpu.VMEM),
        scratch_shapes=[
            pltpu.SMEM(lengths.shape, jnp.int32),
            pltpu.VMEM(queries.shape, BF16),
            pltpu.VMEM(keys.shape, BF16),
            pltpu.VMEM(values.shape, BF16),
            pltpu.VMEM((2, T), jnp.int32),
            pltpu.VMEM((2, T), F32),
            pltpu.VMEM((E, width, ff), BF16),
            pltpu.VMEM((kvl, 2, kv_rows, HD), BF16),
            pltpu.VMEM((E, 2, T), jnp.int32),
            pltpu.VMEM(queries.shape, BF16),
            pltpu.VMEM(queries.shape, BF16),
            pltpu.VMEM((max(1, E // 2 - 1), RB, width), BF16),
            pltpu.VMEM((E, RB, q_rows), BF16),
            pltpu.VMEM((E, RB, width), BF16),
            pltpu.VMEM((S, E, RB, width), BF16),
            pltpu.VMEM((S, RB, ff), F32),
            pltpu.VMEM((S, RB, 1), F32),
            pltpu.VMEM((S * E, RP, nc), BF16),
            pltpu.VMEM((S, E, RP, nc), BF16),
            dma((6,)),
            dma((E,)),
            dma((len(pieces),)),
            dma((len(pieces), kvl)),
            dma((1,)), dma((1,)),
            dma((3,)), dma((E, kvl)),
            dma((1,)), dma((S - 1, E, kvl)),
            dma((1,)), dma((S, len(steps))), dma((kvl,)),
        ],
        compiler_params=pltpu.CompilerParams(
            collective_id=0, has_side_effects=True, vmem_limit_bytes=60 * 1024 * 1024
        ),
    )(*args)


def solution(mesh):
    placed = (
        P(("dp", "seq"), "expert"),
        P(("dp", "seq"), "expert"),
        P(("dp", "seq"), "expert"),
        P("dp"),
        P(("dp", "seq", "expert"), None),
        P(("dp", "seq", "expert"), None),
        P("expert", None, "seq"),
    )
    return jax.shard_map(
        shards,
        mesh=mesh,
        in_specs=placed,
        out_specs=P(("dp", "seq", "expert"), None),
        check_vma=False,
    )
```

```python
import functools

import jax
import jax.numpy as jnp
from jax import lax
from jax.experimental import pallas as pl
from jax.experimental.pallas import tpu as pltpu
from jax.sharding import PartitionSpec as P

HD = 128
MESH = pl.DeviceIdType.MESH
F32 = jnp.float32
BF16 = jnp.bfloat16
NT = (((1,), (1,)), ((), ()))


def up(n, m):
    return -(-n // m) * m


def iota(shape, dim):
    return lax.broadcasted_iota(jnp.int32, shape, dim)


def onehot(mask):
    return jnp.where(mask, F32(1.0), F32(0.0)).astype(BF16)


def dot(a, b):
    return jnp.dot(a, b, preferred_element_type=F32)


def kernel(
    cfg,
    len_hbm, q_hbm, k_hbm, v_hbm, routes_hbm, gates_hbm, w_hbm, out_ref,
    len_ref, q_ref, k_ref, v_ref, routes_ref, gates_ref,
    wbuf, kvbuf, rbuf, raw, nbuf, fwd, sel_ref, pack, xbuf, acc, square_ref, sendbuf, recv,
    in_sem, w_sem, kv_send, kv_recv, r_send, r_recv, z_send, z_recv, x_send, x_recv,
    b_send, b_recv, n_recv, turn,
):
    S, E, ndoc, cap, RB, F, RP, nc, steps, pieces, tile = cfg
    s = lax.axis_index("seq")
    e = lax.axis_index("expert")
    dp = lax.axis_index("dp")
    core = lax.rem(dp, 2)
    partner = {"dp": dp + 1 - 2 * core}
    Q, width = q_ref.shape
    shard = k_ref.shape[0]
    kvl = k_ref.shape[1] // HD
    group = width // HD // kvl
    hw = group * HD
    T = routes_ref.shape[1]
    ff = w_hbm.shape[1]
    depth = w_hbm.shape[0]
    scale = 1.0 / HD**0.5

    def at_s(d):
        return lax.rem(s + S - d, S)

    def at_e(d):
        return lax.rem(e + E - d, E)

    barrier = pltpu.get_barrier_semaphore()
    for ds in range(S):
        for de in range(E):
            if (ds == 0) != (de == 0):
                pl.semaphore_signal(
                    barrier, inc=1, device_id={"seq": at_s(ds), "expert": at_e(de)},
                    device_id_type=MESH,
                )

    pl.semaphore_signal(barrier, inc=1, device_id=partner, device_id_type=MESH)

    mid = (E // 2 - 1, E // 2)

    def key(n, o):
        return (o != n, not (n in mid and o in mid), abs(o - n), o)

    near = [sorted(range(E), key=functools.partial(key, n)) for n in range(E)]
    origin = [e]
    for k in range(1, E):
        o = near[0][k]
        for n in range(1, E):
            o = jnp.where(e == n, near[n][k], o)
        origin.append(o)

    inner_dev = (e == mid[0]) | (e == mid[1])
    side = lax.div(e, E // 2)
    across = E - 1 - e

    def w_copy(k):
        return pltpu.make_async_copy(
            w_hbm.at[pl.ds(pl.multiple_of(origin[k] * width, width), width)],
            wbuf.at[origin[k]], w_sem.at[k],
        )

    ins = []
    for i, (src, dst) in enumerate((
        (k_hbm, k_ref), (q_hbm, q_ref), (v_hbm, v_ref), (len_hbm, len_ref),
        (routes_hbm, routes_ref), (gates_hbm, gates_ref),
    )):
        c = pltpu.make_async_copy(src, dst, in_sem.at[i])
        c.start()
        ins.append(c)
    for c in ins[:5]:
        c.wait()

    def remote(src, dst, ssem, rsem, to_s, to_e):
        return pltpu.make_async_remote_copy(
            src_ref=src, dst_ref=dst, send_sem=ssem, recv_sem=rsem,
            device_id={"seq": to_s, "expert": to_e}, device_id_type=MESH,
        )

    def all_of(ref, sem):
        return pltpu.make_async_copy(ref, ref, sem)

    for k in range(E):
        w_copy(k).start()

    qn = group * Q
    qpos = s * shard + shard - Q + lax.rem(iota((qn, 1), 0), Q)
    docstart = jnp.zeros((qn, 1), jnp.int32)
    begin = jnp.int32(0)
    for j in range(ndoc):
        docstart = jnp.where(qpos >= begin, begin, docstart)
        begin = begin + len_ref[j]

    def masked(q, k, first):
        sc = lax.dot_general(q, k, NT, preferred_element_type=F32) * scale
        kpos = first + iota((1, k.shape[0]), 1)
        return jnp.where((kpos <= qpos) & (kpos >= docstart), sc, F32(-1e30))

    spans = []
    offset = 0
    for d, first in pieces:
        spans.append((offset, shard - first))
        offset += shard - first

    def greet():
        pl.semaphore_wait(barrier, S + E - 1)
        for h in range(kvl):
            for i, (d, first) in enumerate(pieces):
                @pl.when(s + d < S)
                def _():
                    lo, n = spans[i]
                    for j, ref in enumerate((k_ref, v_ref)):
                        remote(
                            ref.at[pl.ds(first, n), pl.ds(h * HD, HD)],
                            kvbuf.at[h, j, pl.ds(lo, n)],
                            kv_send.at[i], kv_recv.at[i, h], s + d, e,
                        ).start()
        for de in range(1, E):
            remote(routes_ref, rbuf.at[de], r_send.at[0], r_recv.at[0], s, at_e(de)).start()

    pl.when(e > 0)(greet)
    queries = []
    local = []
    for h in range(kvl):
        q = jnp.concatenate(
            [q_ref[:, (h * group + g) * HD:(h * group + g + 1) * HD] for g in range(group)], axis=0
        )
        queries.append(q)
        sc = masked(q, k_ref[:, h * HD:(h + 1) * HD], s * shard)
        peak = jnp.max(sc, axis=-1, keepdims=True)
        wt = jnp.exp(sc - peak)
        local.append((peak, jnp.sum(wt, axis=-1, keepdims=True),
                      dot(wt.astype(BF16), v_ref[:, h * HD:(h + 1) * HD])))

    pl.when(e == 0)(greet)

    def part(h):
        return pl.ds(h * hw, hw)

    def relay(src, o, h):
        for ds in range(1, S):
            remote(src, xbuf.at[ds, o, :, part(h)], x_send.at[0], x_recv.at[ds - 1, o, h],
                   at_s(ds), e).start()

    def store_head(h, got, total):
        att = (got / total).astype(BF16)
        for g in range(group):
            cols = slice((h * group + g) * HD, (h * group + g + 1) * HD)
            raw[:, cols] = att[g * Q:(g + 1) * Q]

        @pl.when(inner_dev)
        def _():
            remote(raw.at[:, part(h)], nbuf.at[:, part(h)], z_send.at[1], n_recv.at[h],
                   s, across).start()

    @pl.when(s == 0)
    def _():
        for h in range(kvl):
            store_head(h, local[h][2], local[h][1])

    for h in range(kvl):
        peak, total, got = local[h]

        @pl.when(s > 0)
        def _():
            q = queries[h]
            run_peak, run_total, run_got = peak, total, got
            for i, (d, first) in enumerate(pieces):
                lo, n = spans[i]
                if d > 1:
                    @pl.when(s < d)
                    def _():
                        kvbuf[h, :, lo:lo + n] = jnp.zeros((2, n, HD), BF16)

                @pl.when(s >= d)
                def _():
                    all_of(kvbuf.at[h, :, pl.ds(lo, n)], kv_recv.at[i, h]).wait()

                sc = masked(q, kvbuf[h, 0, lo:lo + n], (s - d) * shard + first)
                higher = jnp.maximum(run_peak, jnp.max(sc, axis=-1, keepdims=True))
                wt = jnp.exp(sc - higher)
                fade = jnp.exp(run_peak - higher)
                run_total = run_total * fade + jnp.sum(wt, axis=-1, keepdims=True)
                run_got = run_got * fade + dot(wt.astype(BF16), kvbuf[h, 1, lo:lo + n])
                run_peak = higher
            store_head(h, run_got, run_total)

    all_of(rbuf.at[pl.ds(1, E - 1)], r_recv.at[0]).wait()
    mine = routes_ref[...]
    names = iota((up(E, 8), 1), 0)
    upper = onehot(iota((T, T), 0) < iota((T, T), 1))
    total_place = jnp.zeros((up(E, 8), Q), F32)
    for de in range(E):
        rt = mine if de == 0 else rbuf[de]
        mt = onehot((rt[0:1, :] == names) | (rt[1:2, :] == names))
        cnt = dot(mt, upper)
        blk = lax.rem(e + de, E)
        place = jnp.where(mt > 0.5, cnt + (blk * cap).astype(F32) + 1.0, F32(0.0))
        if de == 0:
            before = cnt
        shift = onehot(iota((T, Q), 0) + blk * T == iota((T, Q), 1))
        total_place = total_place + dot(place.astype(BF16), shift)
    row_of = iota((RB, Q), 0).astype(F32) + 1.0
    chosen = [onehot(total_place[x:x + 1, :] == row_of) for x in range(E)]
    selector = jnp.concatenate(chosen, axis=0)
    for x in range(E):
        sel_ref[x] = chosen[x]

    def send(k, h):
        to = origin[k]

        @pl.when(jnp.logical_not(inner_dev) | (lax.div(to, E // 2) == side))
        def _():
            remote(pack.at[to, :, part(h)], xbuf.at[0, e, :, part(h)],
                   z_send.at[0], z_recv.at[e, h], s, to).start()

    for h in range(kvl):
        packed = dot(selector, raw[:, h * hw:(h + 1) * hw]).astype(BF16)
        for x in range(E):
            pack[x, :, h * hw:(h + 1) * hw] = packed[x * RB:(x + 1) * RB]
        if h == 0:
            for k in range(1, E - 1):
                send(k, h)
        relay(pack.at[e, :, part(h)], e, h)
    for k in range(1, E):
        for h in range(kvl):
            if h or k == E - 1:
                send(k, h)

    def take_across(o, h):
        all_of(nbuf.at[:, part(h)], n_recv.at[h]).wait()
        rows = nbuf[:, h * hw:(h + 1) * hw]
        for j in range(1, E // 2):
            to = side * (E // 2) + lax.rem(e + j, E // 2)
            fwd[j - 1, :, h * hw:(h + 1) * hw] = dot(sel_ref[to], rows).astype(BF16)
            remote(fwd.at[j - 1, :, part(h)], xbuf.at[0, o, :, part(h)],
                   z_send.at[2], z_recv.at[o, h], s, to).start()
        xbuf[0, o, :, h * hw:(h + 1) * hw] = dot(sel_ref[e], rows).astype(BF16)

    def squares(g, o):
        xf = xbuf[g, o].astype(F32)
        return jnp.sum(xf * xf, axis=-1, keepdims=True)

    square_ref[...] = jnp.zeros_like(square_ref)

    def gather(g, k):
        o = origin[k]
        for h in range(kvl):
            if g:
                all_of(xbuf.at[g, o, :, part(h)], x_recv.at[g - 1, o, h]).wait()
            elif k:
                def direct(o=o, h=h):
                    all_of(xbuf.at[0, o, :, part(h)], z_recv.at[o, h]).wait()

                if k == 1:
                    pl.when(inner_dev)(functools.partial(take_across, o, h))
                    pl.when(jnp.logical_not(inner_dev))(direct)
                else:
                    direct()
                relay(xbuf.at[0, o, :, part(h)], o, h)
        square_ref[g] += squares(g, o)

    def slice_of(g, k):
        if g == 0:
            w_copy(k).wait()
        o = origin[k]
        x = xbuf[g, o]
        for c0 in range(0, ff, tile):
            got = dot(x, wbuf[o, :, c0:c0 + tile])
            acc[g, :, c0:c0 + tile] += got

    xbuf[0, e] = pack[e]
    gather(0, 0)

    rows_out, rows_in = E * RP, F * RB
    out_row = iota((rows_out, 1), 0)
    inner = lax.rem(out_row, RP)
    e_of = lax.rem(e + E - lax.div(out_row, RP), E)
    from_row = lax.div(inner, cap) * RB + e_of * cap + lax.rem(inner, cap)
    from_row = jnp.where(inner < F * cap, from_row, -1)
    perm = onehot(from_row == iota((rows_out, rows_in), 1))

    last = list(range(max(1, E - 2), E))

    def give_back(g):
        factor = lax.rsqrt(square_ref[g] / depth + 1e-05)
        xs = [xbuf[g, origin[k]] for k in last]

        def product(cols):
            total = dot(xs[0], wbuf[origin[last[0]], :, cols])
            for x, k in zip(xs[1:], last[1:]):
                total = total + dot(x, wbuf[origin[k], :, cols])
            return total + acc[g, :, cols]

        to = at_s(S - g) if g else s
        half = (S - g) % S
        for st, (c0, n) in enumerate(steps):
            folded = []
            for f in range(F):
                part = product(slice(f * nc + c0, f * nc + c0 + n)) * factor
                folded.append((part / (1.0 + jnp.exp(-part))).astype(BF16))
            moved = dot(perm, jnp.concatenate(folded, axis=0)).astype(BF16)
            for de in range(E):
                block = moved[de * RP:(de + 1) * RP]
                if g or de:
                    sendbuf[g * E + de, :, c0:c0 + n] = block
                else:
                    recv[0, 0, :, c0:c0 + n] = block
            for de in reversed(range(E)):
                if g or de:
                    c = remote(sendbuf.at[g * E + de, :, pl.ds(c0, n)],
                               recv.at[half, de, :, pl.ds(c0, n)],
                               b_send.at[0], b_recv.at[half, st], to, at_e(de))
                    c.start()

    def others(k):
        for g in range(1, S):
            gather(g, k)
            slice_of(g, k)

    def own_slices(first):
        for g in range(1, S):
            gather(g, 0)
        w_copy(0).wait()
        x = jnp.concatenate([xbuf[g, e] for g in range(S)], axis=0)
        for c0 in range(0, ff, tile):
            got = dot(x, wbuf[e, :, c0:c0 + tile])
            for g in range(S):
                block = got[g * RB:(g + 1) * RB]
                if first or g:
                    acc[g, :, c0:c0 + tile] = block
                else:
                    acc[g, :, c0:c0 + tile] += block

    def middle():
        for k in range(1, last[0]):
            others(k)

    for k in range(1, last[0]):
        gather(0, k)
        if k == 1:
            w_copy(k).wait()
            o = origin[k]
            for c0 in range(0, ff, tile):
                acc[0, :, c0:c0 + tile] = dot(xbuf[0, o], wbuf[o, :, c0:c0 + tile])
            own_slices(False)
        else:
            slice_of(0, k)
    if last[0] == 1:
        own_slices(True)
    pl.when(jnp.logical_not(inner_dev))(middle)
    for k in last[:-1]:
        gather(0, k)
    gather(0, last[-1])
    for k in last:
        w_copy(k).wait()
    def hand():
        @pl.when(core == 0)
        def _():
            pl.semaphore_signal(turn.at[0], inc=1, device_id=partner, device_id_type=MESH)

        @pl.when(core == 1)
        def _():
            pl.semaphore_wait(turn.at[0], 1)

    late = (s > 0) & inner_dev

    @pl.when(jnp.logical_not(late))
    def _():
        give_back(0)
        hand()

    pl.when(inner_dev)(middle)
    for g in range(1, S):
        for k in last:
            gather(g, k)
        give_back(g)

    @pl.when(late)
    def _():
        hand()
        give_back(0)

    ins[5].wait()
    diagonal = iota((T, T), 0) == iota((T, T), 1)

    def column(row):
        return jnp.sum(jnp.where(diagonal, row, jnp.zeros_like(row)), axis=1, keepdims=True)

    wide = iota((T, E * RP), 1)
    at = []
    for k in range(2):
        rk = mine[k:k + 1, :]
        rank = jnp.sum(jnp.where(rk == names, before, F32(0.0)), axis=0, keepdims=True)
        rel = rk - e
        rel = jnp.where(rel < 0, rel + E, rel)
        at.append(column((rel * RP).astype(F32) + rank).astype(jnp.int32))
    pick = jnp.concatenate(
        [onehot(at[k] + f * cap == wide) for f in range(F) for k in range(2)], axis=0
    )
    g0, g1 = column(gates_ref[0:1, :]), column(gates_ref[1:2, :])

    for owner in range(S):
        half = lax.rem(owner + S - s, S)
        for st, (c0, n) in enumerate(steps):
            @pl.when(s == owner)
            def _():
                all_of(recv.at[0, pl.ds(1, E - 1), :, pl.ds(c0, n)], b_recv.at[0, st]).wait()

            @pl.when(s != owner)
            def _():
                all_of(recv.at[half, :, :, pl.ds(c0, n)], b_recv.at[half, st]).wait()

            got = recv[half, :, :, c0:c0 + n].reshape(E * RP, n)
            res = dot(pick, got)
            for f in range(F):
                lo = 2 * f * T
                mix = g0 * res[lo:lo + T] + g1 * res[lo + T:lo + 2 * T]
                cols = slice(owner * ff + f * nc + c0, owner * ff + f * nc + c0 + n)
                out_ref[:, cols] = mix.astype(BF16)

    for i, (d, first) in enumerate(pieces):
        @pl.when(s + d < S)
        def _():
            lo, n = spans[i]
            all_of(kvbuf.at[:, :, pl.ds(lo, n)], kv_send.at[i]).wait()
    all_of(rbuf.at[pl.ds(1, E - 1)], r_send.at[0]).wait()

    @pl.when(jnp.logical_not(inner_dev))
    def _():
        all_of(pack.at[pl.ds(0, E - 1)], z_send.at[0]).wait()

    @pl.when(inner_dev)
    def _():
        all_of(raw, z_send.at[1]).wait()
        if E > 2:
            all_of(pack.at[pl.ds(0, E // 2 - 1)], z_send.at[0]).wait()
            all_of(fwd, z_send.at[2]).wait()

    all_of(xbuf.at[pl.ds(0, S - 1)], x_send.at[0]).wait()
    all_of(sendbuf.at[pl.ds(0, S * E - 1)], b_send.at[0]).wait()


def shards(queries, keys, values, lengths, routes, gates, w_up):
    S, E = lax.axis_size("seq"), lax.axis_size("expert")
    q_rows, width = queries.shape
    shard = keys.shape[0]
    w = w_up.reshape(w_up.shape[1], w_up.shape[2])
    depth, ff = w.shape
    T = routes.shape[0]
    cap = max(2, 3 * q_rows // (E * E))
    choices = [f for f in range(1, ff // 128 + 1) if ff % (f * 128) == 0]
    RB = up(E * cap, 16)
    F = min(choices, key=lambda f: up(f * cap, 16) * (ff // f))
    RP = up(F * cap, 16)
    nc = ff // F
    cuts = list(range(0, max(nc - 255, 1), 256))
    steps = [(c, (cuts + [nc])[i + 1] - c) for i, c in enumerate(cuts)]
    tile = 512 if ff % 512 == 0 else 128
    window = shard * S // 2
    pieces = []
    for d in range(1, S):
        first = max(0, (d + 1) * shard - q_rows - window + 1) // 16 * 16
        if first < shard:
            pieces.append((d, first))
    kv_rows = sum(shard - first for _, first in pieces)
    cfg = (S, E, lengths.shape[0], cap, RB, F, RP, nc, steps, pieces, tile)
    kvl = keys.shape[1] // HD
    dma = pltpu.SemaphoreType.DMA
    args = [
        pltpu.with_memory_space_constraint(a, pltpu.HBM)
        for a in (lengths, queries, keys, values, routes.T, gates.T, w)
    ]
    return pl.pallas_call(
        functools.partial(kernel, cfg),
        out_shape=pltpu.VMEM((T, S * ff), BF16),
        in_specs=[pl.BlockSpec(memory_space=pltpu.HBM)] * 7,
        out_specs=pl.BlockSpec(memory_space=pltpu.VMEM),
        scratch_shapes=[
            pltpu.SMEM(lengths.shape, jnp.int32),
            pltpu.VMEM(queries.shape, BF16),
            pltpu.VMEM(keys.shape, BF16),
            pltpu.VMEM(values.shape, BF16),
            pltpu.VMEM((2, T), jnp.int32),
            pltpu.VMEM((2, T), F32),
            pltpu.VMEM((E, width, ff), BF16),
            pltpu.VMEM((kvl, 2, kv_rows, HD), BF16),
            pltpu.VMEM((E, 2, T), jnp.int32),
            pltpu.VMEM(queries.shape, BF16),
            pltpu.VMEM(queries.shape, BF16),
            pltpu.VMEM((max(1, E // 2 - 1), RB, width), BF16),
            pltpu.VMEM((E, RB, q_rows), BF16),
            pltpu.VMEM((E, RB, width), BF16),
            pltpu.VMEM((S, E, RB, width), BF16),
            pltpu.VMEM((S, RB, ff), F32),
            pltpu.VMEM((S, RB, 1), F32),
            pltpu.VMEM((S * E, RP, nc), BF16),
            pltpu.VMEM((S, E, RP, nc), BF16),
            dma((6,)),
            dma((E,)),
            dma((len(pieces),)),
            dma((len(pieces), kvl)),
            dma((1,)), dma((1,)),
            dma((3,)), dma((E, kvl)),
            dma((1,)), dma((S - 1, E, kvl)),
            dma((1,)), dma((S, len(steps))), dma((kvl,)),
            pltpu.SemaphoreType.REGULAR((1,)),
        ],
        compiler_params=pltpu.CompilerParams(
            collective_id=0, has_side_effects=True, vmem_limit_bytes=60 * 1024 * 1024
        ),
    )(*args)


def solution(mesh):
    placed = (
        P(("dp", "seq"), "expert"),
        P(("dp", "seq"), "expert"),
        P(("dp", "seq"), "expert"),
        P("dp"),
        P(("dp", "seq", "expert"), None),
        P(("dp", "seq", "expert"), None),
        P("expert", None, "seq"),
    )
    return jax.shard_map(
        shards,
        mesh=mesh,
        in_specs=placed,
        out_specs=P(("dp", "seq", "expert"), None),
        check_vma=False,
    )
```

```python
import functools

import jax
import jax.numpy as jnp
from jax import lax
from jax.experimental import pallas as pl
from jax.experimental.pallas import tpu as pltpu
from jax.sharding import PartitionSpec as P

HD = 128
MESH = pl.DeviceIdType.MESH
F32 = jnp.float32
BF16 = jnp.bfloat16
NT = (((1,), (1,)), ((), ()))


def up(n, m):
    return -(-n // m) * m


def iota(shape, dim):
    return lax.broadcasted_iota(jnp.int32, shape, dim)


def onehot(mask):
    return jnp.where(mask, F32(1.0), F32(0.0)).astype(BF16)


def dot(a, b):
    return jnp.dot(a, b, preferred_element_type=F32)


def kernel(
    cfg,
    len_hbm, q_hbm, k_hbm, v_hbm, routes_hbm, gates_hbm, w_hbm, out_ref,
    len_ref, q_ref, k_ref, v_ref, routes_ref, gates_ref,
    wbuf, kvbuf, rbuf, raw, nbuf, fwd, sel_ref, pack, xbuf, acc, square_ref, sendbuf, recv,
    in_sem, w_sem, kv_send, kv_recv, r_send, r_recv, z_send, z_recv, x_send, x_recv,
    b_send, b_recv, n_recv, turn,
):
    S, E, ndoc, cap, RB, F, RP, nc, steps, pieces, tile = cfg
    s = lax.axis_index("seq")
    e = lax.axis_index("expert")
    dp = lax.axis_index("dp")
    core = lax.rem(dp, 2)
    partner = {"dp": dp + 1 - 2 * core}
    Q, width = q_ref.shape
    shard = k_ref.shape[0]
    kvl = k_ref.shape[1] // HD
    group = width // HD // kvl
    hw = group * HD
    T = routes_ref.shape[1]
    ff = w_hbm.shape[1]
    depth = w_hbm.shape[0]
    scale = 1.0 / HD**0.5

    def at_s(d):
        return lax.rem(s + S - d, S)

    def at_e(d):
        return lax.rem(e + E - d, E)

    barrier = pltpu.get_barrier_semaphore()
    for ds in range(S):
        for de in range(E):
            if (ds == 0) != (de == 0):
                pl.semaphore_signal(
                    barrier, inc=1, device_id={"seq": at_s(ds), "expert": at_e(de)},
                    device_id_type=MESH,
                )

    pl.semaphore_signal(barrier, inc=1, device_id=partner, device_id_type=MESH)

    mid = (E // 2 - 1, E // 2)

    def key(n, o):
        return (o != n, not (n in mid and o in mid), abs(o - n), o)

    near = [sorted(range(E), key=functools.partial(key, n)) for n in range(E)]
    origin = [e]
    for k in range(1, E):
        o = near[0][k]
        for n in range(1, E):
            o = jnp.where(e == n, near[n][k], o)
        origin.append(o)

    inner_dev = (e == mid[0]) | (e == mid[1])
    side = lax.div(e, E // 2)
    across = E - 1 - e

    def w_copy(k):
        return pltpu.make_async_copy(
            w_hbm.at[pl.ds(pl.multiple_of(origin[k] * width, width), width)],
            wbuf.at[origin[k]], w_sem.at[k],
        )

    ins = []
    for i, (src, dst) in enumerate((
        (k_hbm, k_ref), (q_hbm, q_ref), (v_hbm, v_ref), (len_hbm, len_ref),
        (routes_hbm, routes_ref), (gates_hbm, gates_ref),
    )):
        c = pltpu.make_async_copy(src, dst, in_sem.at[i])
        c.start()
        ins.append(c)
    for c in ins[:5]:
        c.wait()

    def remote(src, dst, ssem, rsem, to_s, to_e):
        return pltpu.make_async_remote_copy(
            src_ref=src, dst_ref=dst, send_sem=ssem, recv_sem=rsem,
            device_id={"seq": to_s, "expert": to_e}, device_id_type=MESH,
        )

    def all_of(ref, sem):
        return pltpu.make_async_copy(ref, ref, sem)

    for k in range(E):
        w_copy(k).start()

    qn = group * Q
    qpos = s * shard + shard - Q + lax.rem(iota((qn, 1), 0), Q)
    docstart = jnp.zeros((qn, 1), jnp.int32)
    begin = jnp.int32(0)
    for j in range(ndoc):
        docstart = jnp.where(qpos >= begin, begin, docstart)
        begin = begin + len_ref[j]

    def masked(q, k, first):
        sc = lax.dot_general(q, k, NT, preferred_element_type=F32) * scale
        kpos = first + iota((1, k.shape[0]), 1)
        return jnp.where((kpos <= qpos) & (kpos >= docstart), sc, F32(-1e30))

    spans = []
    offset = 0
    for d, first in pieces:
        spans.append((offset, shard - first))
        offset += shard - first

    def greet():
        pl.semaphore_wait(barrier, S + E - 1)
        for h in range(kvl):
            for i, (d, first) in enumerate(pieces):
                @pl.when(s + d < S)
                def _():
                    lo, n = spans[i]
                    for j, ref in enumerate((k_ref, v_ref)):
                        remote(
                            ref.at[pl.ds(first, n), pl.ds(h * HD, HD)],
                            kvbuf.at[h, j, pl.ds(lo, n)],
                            kv_send.at[i], kv_recv.at[i, h], s + d, e,
                        ).start()
        for de in range(1, E):
            remote(routes_ref, rbuf.at[de], r_send.at[0], r_recv.at[0], s, at_e(de)).start()

    pl.when(e > 0)(greet)
    queries = []
    local = []
    for h in range(kvl):
        q = jnp.concatenate(
            [q_ref[:, (h * group + g) * HD:(h * group + g + 1) * HD] for g in range(group)], axis=0
        )
        queries.append(q)
        sc = masked(q, k_ref[:, h * HD:(h + 1) * HD], s * shard)
        peak = jnp.max(sc, axis=-1, keepdims=True)
        wt = jnp.exp(sc - peak)
        local.append((peak, jnp.sum(wt, axis=-1, keepdims=True),
                      dot(wt.astype(BF16), v_ref[:, h * HD:(h + 1) * HD])))

    pl.when(e == 0)(greet)

    def part(h):
        return pl.ds(h * hw, hw)

    def relay(src, o, h):
        for ds in range(1, S):
            remote(src, xbuf.at[ds, o, :, part(h)], x_send.at[0], x_recv.at[ds - 1, o],
                   at_s(ds), e).start()

    def store_head(h, got, total):
        att = (got / total).astype(BF16)
        for g in range(group):
            cols = slice((h * group + g) * HD, (h * group + g + 1) * HD)
            raw[:, cols] = att[g * Q:(g + 1) * Q]

        @pl.when(inner_dev)
        def _():
            remote(raw.at[:, part(h)], nbuf.at[:, part(h)], z_send.at[1], n_recv.at[h],
                   s, across).start()

    @pl.when(s == 0)
    def _():
        for h in range(kvl):
            store_head(h, local[h][2], local[h][1])

    for h in range(kvl):
        peak, total, got = local[h]

        @pl.when(s > 0)
        def _():
            q = queries[h]
            run_peak, run_total, run_got = peak, total, got
            for i, (d, first) in enumerate(pieces):
                lo, n = spans[i]
                if d > 1:
                    @pl.when(s < d)
                    def _():
                        kvbuf[h, :, lo:lo + n] = jnp.zeros((2, n, HD), BF16)

                @pl.when(s >= d)
                def _():
                    all_of(kvbuf.at[h, :, pl.ds(lo, n)], kv_recv.at[i, h]).wait()

                sc = masked(q, kvbuf[h, 0, lo:lo + n], (s - d) * shard + first)
                higher = jnp.maximum(run_peak, jnp.max(sc, axis=-1, keepdims=True))
                wt = jnp.exp(sc - higher)
                fade = jnp.exp(run_peak - higher)
                run_total = run_total * fade + jnp.sum(wt, axis=-1, keepdims=True)
                run_got = run_got * fade + dot(wt.astype(BF16), kvbuf[h, 1, lo:lo + n])
                run_peak = higher
            store_head(h, run_got, run_total)

    all_of(rbuf.at[pl.ds(1, E - 1)], r_recv.at[0]).wait()
    mine = routes_ref[...]
    names = iota((up(E, 8), 1), 0)
    upper = onehot(iota((T, T), 0) < iota((T, T), 1))
    total_place = jnp.zeros((up(E, 8), Q), F32)
    for de in range(E):
        rt = mine if de == 0 else rbuf[de]
        mt = onehot((rt[0:1, :] == names) | (rt[1:2, :] == names))
        cnt = dot(mt, upper)
        blk = lax.rem(e + de, E)
        place = jnp.where(mt > 0.5, cnt + (blk * cap).astype(F32) + 1.0, F32(0.0))
        if de == 0:
            before = cnt
        shift = onehot(iota((T, Q), 0) + blk * T == iota((T, Q), 1))
        total_place = total_place + dot(place.astype(BF16), shift)
    row_of = iota((RB, Q), 0).astype(F32) + 1.0
    chosen = [onehot(total_place[x:x + 1, :] == row_of) for x in range(E)]
    selector = jnp.concatenate(chosen, axis=0)
    for x in range(E):
        sel_ref[x] = chosen[x]

    def send(k, h):
        to = origin[k]

        @pl.when(jnp.logical_not(inner_dev) | (lax.div(to, E // 2) == side))
        def _():
            remote(pack.at[to, :, part(h)], xbuf.at[0, e, :, part(h)],
                   z_send.at[0], z_recv.at[e, h], s, to).start()

    for h in range(kvl):
        packed = dot(selector, raw[:, h * hw:(h + 1) * hw]).astype(BF16)
        for x in range(E):
            pack[x, :, h * hw:(h + 1) * hw] = packed[x * RB:(x + 1) * RB]
        if h == 0:
            for k in range(1, E - 1):
                send(k, h)
        relay(pack.at[e, :, part(h)], e, h)
    for k in range(1, E):
        for h in range(kvl):
            if h or k == E - 1:
                send(k, h)

    def take_across(o, h):
        all_of(nbuf.at[:, part(h)], n_recv.at[h]).wait()
        rows = nbuf[:, h * hw:(h + 1) * hw]
        for j in range(1, E // 2):
            to = side * (E // 2) + lax.rem(e + j, E // 2)
            fwd[j - 1, :, h * hw:(h + 1) * hw] = dot(sel_ref[to], rows).astype(BF16)
            remote(fwd.at[j - 1, :, part(h)], xbuf.at[0, o, :, part(h)],
                   z_send.at[2], z_recv.at[o, h], s, to).start()
        xbuf[0, o, :, h * hw:(h + 1) * hw] = dot(sel_ref[e], rows).astype(BF16)

    def squares(g, o):
        xf = xbuf[g, o].astype(F32)
        return jnp.sum(xf * xf, axis=-1, keepdims=True)

    square_ref[...] = jnp.zeros_like(square_ref)

    def gather(g, k):
        o = origin[k]
        if g:
            all_of(xbuf.at[g, o], x_recv.at[g - 1, o]).wait()
        for h in range(kvl):
            if k and not g:
                def direct(o=o, h=h):
                    all_of(xbuf.at[0, o, :, part(h)], z_recv.at[o, h]).wait()

                if k == 1:
                    pl.when(inner_dev)(functools.partial(take_across, o, h))
                    pl.when(jnp.logical_not(inner_dev))(direct)
                else:
                    direct()
                relay(xbuf.at[0, o, :, part(h)], o, h)
        square_ref[g] += squares(g, o)

    def slice_of(g, k):
        if g == 0:
            w_copy(k).wait()
        o = origin[k]
        x = xbuf[g, o]
        for c0 in range(0, ff, tile):
            got = dot(x, wbuf[o, :, c0:c0 + tile])
            acc[g, :, c0:c0 + tile] += got

    xbuf[0, e] = pack[e]
    gather(0, 0)

    rows_out, rows_in = E * RP, F * RB
    out_row = iota((rows_out, 1), 0)
    inner = lax.rem(out_row, RP)
    e_of = lax.rem(e + E - lax.div(out_row, RP), E)
    from_row = lax.div(inner, cap) * RB + e_of * cap + lax.rem(inner, cap)
    from_row = jnp.where(inner < F * cap, from_row, -1)
    perm = onehot(from_row == iota((rows_out, rows_in), 1))

    last = list(range(max(1, E - 2), E))

    def hand():
        @pl.when(core == 0)
        def _():
            pl.semaphore_signal(turn.at[0], inc=1, device_id=partner, device_id_type=MESH)

        @pl.when(core == 1)
        def _():
            pl.semaphore_wait(turn.at[0], 1)

    late = (s > 0) & inner_dev

    def give_back(g, leads=None):
        factor = lax.rsqrt(square_ref[g] / depth + 1e-05)
        xs = [xbuf[g, origin[k]] for k in last]

        def product(cols):
            total = dot(xs[0], wbuf[origin[last[0]], :, cols])
            for x, k in zip(xs[1:], last[1:]):
                total = total + dot(x, wbuf[origin[k], :, cols])
            return total + acc[g, :, cols]

        to = at_s(S - g) if g else s
        half = (S - g) % S
        for st, (c0, n) in enumerate(steps):
            folded = []
            for f in range(F):
                part = product(slice(f * nc + c0, f * nc + c0 + n)) * factor
                folded.append((part / (1.0 + jnp.exp(-part))).astype(BF16))
            moved = dot(perm, jnp.concatenate(folded, axis=0)).astype(BF16)
            for de in range(E):
                block = moved[de * RP:(de + 1) * RP]
                if g or de:
                    sendbuf[g * E + de, :, c0:c0 + n] = block
                else:
                    recv[0, 0, :, c0:c0 + n] = block
            for de in reversed(range(E)):
                if g or de:
                    c = remote(sendbuf.at[g * E + de, :, pl.ds(c0, n)],
                               recv.at[half, de, :, pl.ds(c0, n)],
                               b_send.at[0], b_recv.at[half, st], to, at_e(de))
                    c.start()
            if leads is not None and st == 1:
                pl.when(leads & (core == 0))(hand)

    def others(k):
        for g in range(1, S):
            gather(g, k)
            slice_of(g, k)

    def own_slices(first):
        for g in range(1, S):
            gather(g, 0)
        w_copy(0).wait()
        x = jnp.concatenate([xbuf[g, e] for g in range(S)], axis=0)
        for c0 in range(0, ff, tile):
            got = dot(x, wbuf[e, :, c0:c0 + tile])
            for g in range(S):
                block = got[g * RB:(g + 1) * RB]
                if first or g:
                    acc[g, :, c0:c0 + tile] = block
                else:
                    acc[g, :, c0:c0 + tile] += block

    def middle():
        for k in range(1, last[0]):
            others(k)

    for k in range(1, last[0]):
        gather(0, k)
        if k == 1:
            w_copy(k).wait()
            o = origin[k]
            for c0 in range(0, ff, tile):
                acc[0, :, c0:c0 + tile] = dot(xbuf[0, o], wbuf[o, :, c0:c0 + tile])
            own_slices(False)
        else:
            slice_of(0, k)
    if last[0] == 1:
        own_slices(True)
    pl.when(jnp.logical_not(inner_dev))(middle)
    for k in last[:-1]:
        gather(0, k)
    gather(0, last[-1])
    for k in last:
        w_copy(k).wait()

    @pl.when(jnp.logical_not(late))
    def _():
        give_back(0, s >= 0)
        pl.when(core == 1)(hand)

    pl.when(inner_dev)(middle)
    for g in range(1, S):
        for k in last:
            gather(g, k)
        give_back(g, late if g == S - 1 else None)

    @pl.when(late)
    def _():
        pl.when(core == 1)(hand)
        give_back(0)

    ins[5].wait()
    diagonal = iota((T, T), 0) == iota((T, T), 1)

    def column(row):
        return jnp.sum(jnp.where(diagonal, row, jnp.zeros_like(row)), axis=1, keepdims=True)

    wide = iota((T, E * RP), 1)
    at = []
    for k in range(2):
        rk = mine[k:k + 1, :]
        rank = jnp.sum(jnp.where(rk == names, before, F32(0.0)), axis=0, keepdims=True)
        rel = rk - e
        rel = jnp.where(rel < 0, rel + E, rel)
        at.append(column((rel * RP).astype(F32) + rank).astype(jnp.int32))
    pick = jnp.concatenate(
        [onehot(at[k] + f * cap == wide) for f in range(F) for k in range(2)], axis=0
    )
    g0, g1 = column(gates_ref[0:1, :]), column(gates_ref[1:2, :])

    for owner in range(S):
        half = lax.rem(owner + S - s, S)
        for st, (c0, n) in enumerate(steps):
            @pl.when(s == owner)
            def _():
                all_of(recv.at[0, pl.ds(1, E - 1), :, pl.ds(c0, n)], b_recv.at[0, st]).wait()

            @pl.when(s != owner)
            def _():
                all_of(recv.at[half, :, :, pl.ds(c0, n)], b_recv.at[half, st]).wait()

            got = recv[half, :, :, c0:c0 + n].reshape(E * RP, n)
            res = dot(pick, got)
            for f in range(F):
                lo = 2 * f * T
                mix = g0 * res[lo:lo + T] + g1 * res[lo + T:lo + 2 * T]
                cols = slice(owner * ff + f * nc + c0, owner * ff + f * nc + c0 + n)
                out_ref[:, cols] = mix.astype(BF16)

    for i, (d, first) in enumerate(pieces):
        @pl.when(s + d < S)
        def _():
            lo, n = spans[i]
            all_of(kvbuf.at[:, :, pl.ds(lo, n)], kv_send.at[i]).wait()
    all_of(rbuf.at[pl.ds(1, E - 1)], r_send.at[0]).wait()

    @pl.when(jnp.logical_not(inner_dev))
    def _():
        all_of(pack.at[pl.ds(0, E - 1)], z_send.at[0]).wait()

    @pl.when(inner_dev)
    def _():
        all_of(raw, z_send.at[1]).wait()
        if E > 2:
            all_of(pack.at[pl.ds(0, E // 2 - 1)], z_send.at[0]).wait()
            all_of(fwd, z_send.at[2]).wait()

    all_of(xbuf.at[pl.ds(0, S - 1)], x_send.at[0]).wait()
    all_of(sendbuf.at[pl.ds(0, S * E - 1)], b_send.at[0]).wait()


def shards(queries, keys, values, lengths, routes, gates, w_up):
    S, E = lax.axis_size("seq"), lax.axis_size("expert")
    q_rows, width = queries.shape
    shard = keys.shape[0]
    w = w_up.reshape(w_up.shape[1], w_up.shape[2])
    depth, ff = w.shape
    T = routes.shape[0]
    cap = max(2, 3 * q_rows // (E * E))
    choices = [f for f in range(1, ff // 128 + 1) if ff % (f * 128) == 0]
    RB = up(E * cap, 16)
    F = min(choices, key=lambda f: up(f * cap, 16) * (ff // f))
    RP = up(F * cap, 16)
    nc = ff // F
    cuts = list(range(0, max(nc - 255, 1), 256))
    steps = [(c, (cuts + [nc])[i + 1] - c) for i, c in enumerate(cuts)]
    tile = 512 if ff % 512 == 0 else 128
    window = shard * S // 2
    pieces = []
    for d in range(1, S):
        first = max(0, (d + 1) * shard - q_rows - window + 1) // 16 * 16
        if first < shard:
            pieces.append((d, first))
    kv_rows = sum(shard - first for _, first in pieces)
    cfg = (S, E, lengths.shape[0], cap, RB, F, RP, nc, steps, pieces, tile)
    kvl = keys.shape[1] // HD
    dma = pltpu.SemaphoreType.DMA
    args = [
        pltpu.with_memory_space_constraint(a, pltpu.HBM)
        for a in (lengths, queries, keys, values, routes.T, gates.T, w)
    ]
    return pl.pallas_call(
        functools.partial(kernel, cfg),
        out_shape=pltpu.VMEM((T, S * ff), BF16),
        in_specs=[pl.BlockSpec(memory_space=pltpu.HBM)] * 7,
        out_specs=pl.BlockSpec(memory_space=pltpu.VMEM),
        scratch_shapes=[
            pltpu.SMEM(lengths.shape, jnp.int32),
            pltpu.VMEM(queries.shape, BF16),
            pltpu.VMEM(keys.shape, BF16),
            pltpu.VMEM(values.shape, BF16),
            pltpu.VMEM((2, T), jnp.int32),
            pltpu.VMEM((2, T), F32),
            pltpu.VMEM((E, width, ff), BF16),
            pltpu.VMEM((kvl, 2, kv_rows, HD), BF16),
            pltpu.VMEM((E, 2, T), jnp.int32),
            pltpu.VMEM(queries.shape, BF16),
            pltpu.VMEM(queries.shape, BF16),
            pltpu.VMEM((max(1, E // 2 - 1), RB, width), BF16),
            pltpu.VMEM((E, RB, q_rows), BF16),
            pltpu.VMEM((E, RB, width), BF16),
            pltpu.VMEM((S, E, RB, width), BF16),
            pltpu.VMEM((S, RB, ff), F32),
            pltpu.VMEM((S, RB, 1), F32),
            pltpu.VMEM((S * E, RP, nc), BF16),
            pltpu.VMEM((S, E, RP, nc), BF16),
            dma((6,)),
            dma((E,)),
            dma((len(pieces),)),
            dma((len(pieces), kvl)),
            dma((1,)), dma((1,)),
            dma((3,)), dma((E, kvl)),
            dma((1,)), dma((S - 1, E)),
            dma((1,)), dma((S, len(steps))), dma((kvl,)),
            pltpu.SemaphoreType.REGULAR((1,)),
        ],
        compiler_params=pltpu.CompilerParams(
            collective_id=0, has_side_effects=True, vmem_limit_bytes=60 * 1024 * 1024
        ),
    )(*args)


def solution(mesh):
    placed = (
        P(("dp", "seq"), "expert"),
        P(("dp", "seq"), "expert"),
        P(("dp", "seq"), "expert"),
        P("dp"),
        P(("dp", "seq", "expert"), None),
        P(("dp", "seq", "expert"), None),
        P("expert", None, "seq"),
    )
    return jax.shard_map(
        shards,
        mesh=mesh,
        in_specs=placed,
        out_specs=P(("dp", "seq", "expert"), None),
        check_vma=False,
    )
```
